32 devices in a mesh: dp: 1 (over z), tp: 32 (over x, y, core).
Axes of the slice: x: 4, y: 4, z: 1, core: 2. Of those that a mesh axis runs over, the one named last changes fastest.
The devices are a block of a 4x4x8 slice.
Arguments:
- x: bfloat16 [4096, 8192], P(('dp', 'tp'))
- dy: bfloat16 [4096, 8192], P(('dp', 'tp'))
- pre: bfloat16 [4096, 32768], P('dp', 'tp')
- w_in: bfloat16 [8192, 32768], P(None, 'tp')
- w_down: bfloat16 [32768, 8192], P('tp')
Outputs:
- output 1: bfloat16 [4096, 8192], P(('dp', 'tp'))
- output 2: bfloat16 [8192, 32768], P('dp', 'tp')
- output 3: bfloat16 [32768, 8192], P(('dp', 'tp'))
All inputs are finite; a program needn't handle non-finite values.
Results may differ from the reference program's by a relative error of at most 0.012.
Values are sent between devices in bfloat16 or wider.
A program may use at most 768 MiB of HBM per device.

```python
import jax
import jax.numpy as jnp

ROWS = 4096
D = 8192
FF = 32768


def act(pre):
    return jax.nn.gelu(pre)


def setup_inputs(seed: int = 0, part: int = 0) -> dict:
    kx, ky, ka, ki, kd = jax.random.split(jax.random.key(seed), 5)
    kx, ky, ka = (jax.random.fold_in(k, part) for k in (kx, ky, ka))
    drawn = {
        "x": jax.random.normal(kx, (ROWS, D), jnp.float32),
        "dy": jax.random.normal(ky, (ROWS, D), jnp.float32),
        "pre": jax.random.normal(ka, (ROWS, FF), jnp.float32),
        "w_in": jax.random.normal(ki, (D, FF), jnp.float32) * D**-0.5,
        "w_down": jax.random.normal(kd, (FF, D), jnp.float32) * FF**-0.5,
    }
    return {k: v.astype(jnp.bfloat16) for k, v in drawn.items()}


def reference(x, dy, pre, w_in, w_down):
    hidden, back = jax.vjp(act, pre.astype(jnp.float32))
    d_hidden = jnp.dot(dy, w_down.T, preferred_element_type=jnp.float32)
    d_pre = back(d_hidden)[0].astype(jnp.bfloat16)
    dx = jnp.dot(d_pre, w_in.T, preferred_element_type=jnp.float32)
    dw_in = jnp.dot(x.T, d_pre, preferred_element_type=jnp.float32)
    dw_down = jnp.dot(hidden.astype(jnp.bfloat16).T, dy, preferred_element_type=jnp.float32)
    return tuple(g.astype(jnp.bfloat16) for g in (dx, dw_in, dw_down))
```

```python
import functools
import math

import jax
import jax.numpy as jnp
from jax import lax
from jax.experimental import pallas as pl
from jax.experimental.pallas import tpu as pltpu
from jax.sharding import PartitionSpec as P

MESH = pl.DeviceIdType.MESH
F32, BF16 = jnp.float32, jnp.bfloat16
SUB = 4
TILE = 256


def ring_pos(side, chip, ring):
    a, b = chip // side, chip % side
    return jnp.where(ring == 0, a, b) * side + (a + b) % side


def ring_chip(side, pos, ring):
    pos = (pos + side * side) % (side * side)
    major = pos // side
    minor = (pos % side - major + side) % side
    return jnp.where(ring == 0, major * side + minor, minor * side + major)


def dot(a, b, ca, cb):
    return lax.dot_general(a, b, (((ca,), (cb,)), ((), ())), preferred_element_type=F32)


def gelu_and_slope(p):
    c = math.sqrt(2.0 / math.pi)
    sq = p * p
    t = jnp.tanh(c * (p + 0.044715 * (sq * p)))
    cdf = 0.5 * (1.0 + t)
    slope = cdf + p * (0.5 * (1.0 - t * t)) * (c * (1.0 + 3 * 0.044715 * sq))
    return p * cdf, slope


def kernel(n, x, dy, pre, w_in, w_down, dx, dw_in, dw_down, gb, rsb, sbb, dpre, w2,
           agr, ags, d2r, d2s, rsr, rss, sbr, sbs, wsem, psem, osem, lsem, tsem):
    S = n // 2
    side = math.isqrt(S)
    R, D = x.shape
    H, Q, F = R // 2, R // 2 // SUB, pre.shape[1]
    DC = D // SUB
    NT = D // TILE
    me = lax.axis_index("tp")
    chip, core = me // 2, me % 2
    pos, pos2 = ring_pos(side, chip, core), ring_pos(side, chip, 1 - core)
    nxt = [ring_chip(side, pos + 1, core) * 2 + core, ring_chip(side, pos - 1, core) * 2 + core]
    sib = chip * 2 + 1 - core

    def remote(src, dst, ssem, rsem, dev):
        return pltpu.make_async_remote_copy(src, dst, ssem, rsem, device_id={"tp": dev}, device_id_type=MESH)

    def land(v):
        return v + v // (S - 1)

    def ag_copy(v, d, q, src=None):
        rows = pl.ds(d * H + q * Q, Q)
        slot = jnp.where(v % (S - 1) == 0, land(v) + S - 1, land(v) - 1)
        src = gb.at[0, slot, rows] if src is None else src.at[rows]
        return remote(src, gb.at[0, land(v), rows], ags.at[v], agr.at[v, d, q], nxt[d])

    def pump(v, q, last=False):
        for d in range(2):
            ag_copy(v, d, q).wait_recv()
            if not last:
                ag_copy(v + 1, d, q).start()

    def d2d(w, src=None):
        return remote(gb.at[0, w] if src is None else src, gb.at[1, w], d2s.at[w], d2r.at[w], sib)

    bar = pltpu.get_barrier_semaphore()
    for dev in (*nxt, sib):
        pl.semaphore_signal(bar, inc=1, device_id={"tp": dev}, device_id_type=MESH)
    pl.semaphore_wait(bar, 3)
    for q in range(SUB):
        for d in range(2):
            ag_copy(0, d, q, dy).start()
    d2d(S - 1, dy).start()
    d2d(2 * S - 1, x).start()
    load_w2 = pltpu.make_async_copy(w_in, w2, wsem.at[1])

    def first(hT):
        def p1(w1, a, prb):
            load_w1 = pltpu.make_async_copy(w_down, w1, wsem.at[0])
            own = [pltpu.make_async_copy(dy, a.at[0], lsem.at[0]), pltpu.make_async_copy(x, a.at[1], lsem.at[1])]
            put = [pltpu.make_async_copy(a.at[0], gb.at[0, S - 1], lsem.at[0]),
                   pltpu.make_async_copy(a.at[1], gb.at[0, 2 * S - 1], lsem.at[1])]
            for c in own:
                c.start()
            load_w1.start()
            load_w2.start()
            for o, c in zip(own, put):
                o.wait()
                c.start()
            for c in put:
                c.wait()

            def loads(e):
                out = [pltpu.make_async_copy(gb.at[:, e], a, lsem.at[0])]
                for h, (ps, cr) in enumerate(((pos, core), (pos2, 1 - core))):
                    for d in range(2):
                        c = ring_chip(side, ps + (e + 1 if d else 2 * S - 1 - e), cr)
                        row = pl.multiple_of((c * 2 + cr) * R + d * H, H)
                        out.append(pltpu.make_async_copy(pre.at[pl.ds(row, H)], prb.at[h, pl.ds(d * H, H)], psem.at[h, d]))
                return out

            @pl.loop(0, S + 1)
            def _(v):
                @pl.when(v == 1)
                def _():
                    load_w1.wait()

                e = (v + S - 2) % S

                @pl.loop(0, SUB)
                def _(q):
                    pump(v, q)

                    @pl.when(v >= 1)
                    def _():
                        @pl.when(q == 0)
                        def _():
                            for c in loads(e):
                                c.wait()

                        FC = F // SUB
                        cols = pl.ds(pl.multiple_of(q * FC, FC), FC)
                        dh = dot(a[...].reshape(2 * R, D), w1[cols, :], 1, 1)
                        for h in range(2):
                            hid, slope = gelu_and_slope(prb[h, :, cols].astype(F32))
                            dpre[h, e, :, cols] = (dh[h * R : (h + 1) * R] * slope).astype(BF16)
                            tok = pl.ds(pl.multiple_of((h * S + e) * R, R), R)
                            hT[cols, tok] = hid.T.astype(BF16)

                d2d(land(v)).start()

                @pl.when(v < S)
                def _():
                    e1 = (v + S - 1) % S
                    d2d(e1).wait_recv()
                    for c in loads(e1):
                        c.start()

        pl.run_scoped(p1, pltpu.VMEM((F, D), BF16), pltpu.VMEM((2, R, D), BF16), pltpu.VMEM((2, R, F), BF16))

        def p2(tile, dout, sst):
            load_w2.wait()

            def tile_load(i):
                cols = pl.ds(pl.multiple_of(i * TILE, TILE), TILE)
                return pltpu.make_async_copy(gb.at[:, pl.ds(0, S), :, cols], tile.at[i % 2], tsem.at[i % 2])

            def tile_out(i):
                cols = pl.ds(pl.multiple_of(i * TILE, TILE), TILE)
                return pltpu.make_async_copy(dout.at[i % 2], dw_down.at[:, cols], osem.at[i % 2])

            def sib_copy(k, c):
                return remote(sst.at[k % 2, c], sbb.at[k, c], sbs.at[k % 2, c], sbr.at[k, c], sib)

            tile_load(0).start()

            @pl.loop(0, S)
            def _(g):
                def step(u):
                    v = S + 1 + u // SUB
                    pump(v, u % SUB)

                    @pl.when(u % SUB == SUB - 1)
                    def _():
                        d2d(land(v)).start()

                @pl.loop(0, 2)
                def _(j):
                    step(3 * g + j)
                    i = 2 * g + j
                    tile_load(i).wait()

                    @pl.when(i + 1 < NT)
                    def _():
                        tile_load(i + 1).start()

                    @pl.when(i >= 2)
                    def _():
                        tile_out(i - 2).wait()

                    dout[i % 2] = dot(hT[...], tile[i % 2].reshape(2 * S * R, TILE), 1, 0).astype(BF16)
                    tile_out(i).start()

                step(3 * g + 2)

                @pl.loop(0, 2)
                def _(j):
                    k, c = g // 2, (g % 2) * 2 + j

                    @pl.when(k >= 2)
                    def _():
                        sib_copy(k - 2, c).wait_send()

                    part = dot(dpre[1, pl.ds(2 * k, 2)].reshape(2 * R, F), w2[pl.ds(pl.multiple_of(c * DC, DC), DC), :], 1, 1)
                    sst[k % 2, c] = part.astype(BF16).reshape(2, R, DC)
                    sib_copy(k, c).start()

            for i in range(NT - 2, NT):
                tile_out(i).wait()

            @pl.loop(S // 2 - 2, S // 2)
            def _(k):
                for c in range(SUB):
                    sib_copy(k, c).wait_send()

        pl.run_scoped(p2, pltpu.VMEM((2, 2, S, R, TILE), BF16), pltpu.VMEM((2, F, TILE), BF16), pltpu.VMEM((2, SUB, 2, R, DC), BF16))

    pl.run_scoped(first, pltpu.VMEM((F, 2 * S * R), BF16))

    def p3(own, xt, eo, got, gsib, out):
        last = 2 * (S - 1) - 1

        def x_load(i):
            cols = pl.ds(pl.multiple_of(i * TILE, TILE), TILE)
            return pltpu.make_async_copy(gb.at[:, pl.ds(S, S), :, cols], xt.at[i % 2], tsem.at[i % 2])

        def e_out(i):
            return pltpu.make_async_copy(eo.at[i % 2], dw_in.at[pl.ds(pl.multiple_of(i * TILE, TILE), TILE)], osem.at[i % 2])

        def rs_copy(s, d, q):
            rows = pl.ds(d * H, H)
            return remote(out.at[s % 2, q, rows], rsb.at[s, q, rows], rss.at[s % 2, d, q], rsr.at[s, d, q], nxt[d])

        def got_load(s, q):
            return pltpu.make_async_copy(rsb.at[s - 1, q], got.at[q % 2], lsem.at[q % 2])

        def sib_load(s, q):
            return pltpu.make_async_copy(sbb.at[s // 2, q, s % 2], gsib.at[q % 2], psem.at[0, q % 2])

        def sib_arrive(s, q):
            @pl.when(s % 2 == 0)
            def _():
                remote(sbb.at[s // 2, q], sbb.at[s // 2, q], sbs.at[0, q], sbr.at[s // 2, q], sib).wait_recv()

        def dx_out(q):
            return pltpu.make_async_copy(out.at[(S - 1) % 2, q], dx.at[:, pl.ds(pl.multiple_of(q * DC, DC), DC)], tsem.at[2 + q])

        sib_arrive(0, 0)
        sib_load(0, 0).start()

        @pl.loop(0, S)
        def _(s):
            @pl.loop(0, SUB)
            def _(q):
                @pl.when(s % 2 == 0)
                def _():
                    part = dot(dpre[0, pl.ds(s, 2)].reshape(2 * R, F), w2[pl.ds(pl.multiple_of(q * DC, DC), DC), :], 1, 1)
                    own[q] = part.reshape(2, R, DC)

                @pl.when(s >= 2)
                def _():
                    for d in range(2):
                        rs_copy(s - 2, d, q).wait_send()

                sib_load(s, q).wait()

                @pl.when(s == 0)
                def _():
                    out[s % 2, q] = (own[q, s % 2] + gsib[q % 2].astype(F32)).astype(BF16)

                @pl.when(s > 0)
                def _():
                    got_load(s, q).wait()
                    out[s % 2, q] = (own[q, s % 2] + gsib[q % 2].astype(F32) + got[q % 2].astype(F32)).astype(BF16)

                @pl.when(s < S - 1)
                def _():
                    for d in range(2):
                        rs_copy(s, d, q).start()

                @pl.when(s == S - 1)
                def _():
                    dx_out(q).start()

                @pl.when(s == 0)
                def _():
                    pump(last, q, True)

                @pl.when((s == 0) & (q == SUB - 1))
                def _():
                    d2d(land(last)).start()

                @pl.when((s < S - 1) | (q < SUB - 1))
                def _():
                    q1 = (q + 1) % SUB
                    s1 = s + (q + 1) // SUB
                    sib_arrive(s1, q1)
                    sib_load(s1, q1).start()

                    @pl.when(s1 > 0)
                    def _():
                        for d in range(2):
                            rs_copy(s1 - 1, d, q1).wait_recv()
                        got_load(s1, q1).start()

                @pl.when(s % 2 == 1)
                def _():
                    i = (s // 2) * SUB + q

                    @pl.when(i == 0)
                    def _():
                        @pl.loop(S, 2 * S)
                        def _(w):
                            d2d(w).wait_recv()

                        x_load(0).start()

                    x_load(i).wait()

                    @pl.when(i + 1 < NT)
                    def _():
                        x_load(i + 1).start()

                    @pl.when(i >= 2)
                    def _():
                        e_out(i - 2).wait()

                    eo[i % 2] = dot(xt[i % 2].reshape(2 * S * R, TILE), dpre[...].reshape(2 * S * R, F), 0, 0).astype(BF16)
                    e_out(i).start()

        for i in range(NT - 2, NT):
            e_out(i).wait()
        for q in range(SUB):
            for d in range(2):
                rs_copy(S - 2, d, q).wait_send()
            dx_out(q).wait()

    pl.run_scoped(p3, pltpu.VMEM((SUB, 2, R, DC), F32), pltpu.VMEM((2, 2, S, R, TILE), BF16), pltpu.VMEM((2, TILE, F), BF16),
                  pltpu.VMEM((2, R, DC), BF16), pltpu.VMEM((2, R, DC), BF16), pltpu.VMEM((2, SUB, R, DC), BF16))

    @pl.loop(0, 2 * (S - 1))
    def _(v):
        remote(gb.at[0, 0], gb.at[0, 0], ags.at[v], agr.at[v, 0, 0], nxt[0]).wait_send()

    @pl.loop(0, 2 * S)
    def _(w):
        d2d(w).wait_send()


def solution(mesh):
    n = mesh.shape["tp"]
    S = n // 2

    def step(x, dy, pre, w_in, w_down):
        R, D = x.shape
        F = pre.shape[1]
        sds = jax.ShapeDtypeStruct
        dma = pltpu.SemaphoreType.DMA
        dx, dw_in, dw_down, *_ = pl.pallas_call(
            functools.partial(kernel, n),
            out_shape=(
                sds((R, D), BF16), sds((D, F), BF16), sds((F, D), BF16),
                sds((2, 2 * S, R, D), BF16), sds((S - 1, SUB, R, D // SUB), BF16), sds((S // 2, SUB, 2, R, D // SUB), BF16),
            ),
            in_specs=[pl.BlockSpec(memory_space=pl.ANY)] * 5,
            out_specs=[pl.BlockSpec(memory_space=pl.ANY)] * 6,
            scratch_shapes=[
                pltpu.VMEM((2, S, R, F), BF16), pltpu.VMEM((D, F), BF16),
                dma((2 * (S - 1), 2, SUB)), dma((2 * (S - 1),)), dma((2 * S,)), dma((2 * S,)),
                dma((S - 1, 2, SUB)), dma((2, 2, SUB)), dma((S // 2, SUB)), dma((2, SUB)),
                dma((2,)), dma((2, 2)), dma((2,)), dma((2,)), dma((2 + SUB,)),
            ],
            compiler_params=pltpu.CompilerParams(collective_id=0, has_side_effects=True, vmem_limit_bytes=63 * 2**20),
            name="mlp_backward",
        )(x, dy, pre, w_in, w_down)
        return dx, dw_in, dw_down

    rows, cols = P(("dp", "tp"), None), P("dp", "tp")
    return jax.shard_map(
        step, mesh=mesh, in_specs=(rows, rows, cols, P(None, "tp"), P("tp", None)),
        out_specs=(rows, cols, rows), check_vma=False,
    )
```

```python
import functools
import math

import jax
import jax.numpy as jnp
from jax import lax
from jax.experimental import pallas as pl
from jax.experimental.pallas import tpu as pltpu
from jax.sharding import PartitionSpec as P

MESH = pl.DeviceIdType.MESH
F32, BF16 = jnp.float32, jnp.bfloat16
SUB = 4
TILE = 256
VMEM_LIMIT = 63 * 2**20


def ring_pos(side, chip, ring):
    a, b = chip // side, chip % side
    return jnp.where(ring == 0, a, b) * side + (a + b) % side


def ring_chip(side, pos, ring):
    pos = (pos + side * side) % (side * side)
    major = pos // side
    minor = (pos % side - major + side) % side
    return jnp.where(ring == 0, major * side + minor, minor * side + major)


def ring_perms(n):
    S = n // 2
    side = math.isqrt(S)
    with jax.ensure_compile_time_eval():
        ring = [[int(ring_chip(side, p, c)) * 2 + c for p in range(S)] for c in range(2)]
    return [[(r[p], r[(p + d) % S]) for r in ring for p in range(S)] for d in (1, -1)]


def dot(a, b, ca, cb):
    return lax.dot_general(a, b, (((ca,), (cb,)), ((), ())), preferred_element_type=F32)


def gelu_and_slope(p):
    c = math.sqrt(2.0 / math.pi)
    sq = p * p
    t = jnp.tanh(c * (p + 0.044715 * (sq * p)))
    cdf = 0.5 * (1.0 + t)
    slope = cdf + p * (0.5 * (1.0 - t * t)) * (c * (1.0 + 3 * 0.044715 * sq))
    return p * cdf, slope


def kernel(n, x, dy, pre, w_in, w_down, snd0, snd1, terms, dw_in, dw_down, gb, rsb, sbb, dpre, w2,
           agr, ags, d2r, d2s, rsr, rss, sbr, sbs, wsem, psem, osem, lsem, tsem, fsem):
    S = n // 2
    G = S // 2
    side = math.isqrt(S)
    R, D = x.shape
    H, Q, F = R // 2, R // SUB, pre.shape[1]
    DC, FC = D // SUB, F // SUB
    NT = D // TILE
    me = lax.axis_index("tp")
    chip, core = me // 2, me % 2
    pos, pos2 = ring_pos(side, chip, core), ring_pos(side, chip, 1 - core)
    nxt = [ring_chip(side, pos + 1, core) * 2 + core, ring_chip(side, pos - 1, core) * 2 + core]
    sib = chip * 2 + 1 - core

    def remote(src, dst, ssem, rsem, dev):
        return pltpu.make_async_remote_copy(src, dst, ssem, rsem, device_id={"tp": dev}, device_id_type=MESH)

    def land(v, d):
        return S * (v // G) + jnp.where(v % G == G - 1, S - 2, 2 * (v % G) + d)

    def ag_copy(v, d, q, src=None):
        rows = pl.ds(q * Q if isinstance(q, int) else pl.multiple_of(q * Q, Q), Q)
        slot = S * (v // G) + jnp.where(v % G == 0, S - 1, 2 * (v % G - 1) + d)
        src = gb.at[0, slot, rows] if src is None else src.at[rows]
        return remote(src, gb.at[0, land(v, d), rows], ags.at[v, d], agr.at[v, d, q], nxt[d])

    def goes(v, d, q):
        return (v % G < G - 1) | ((q >= SUB // 2) if d else (q < SUB // 2))

    def d2d_part(w, q):
        rows = pl.ds(pl.multiple_of(q * Q, Q), Q)
        return remote(gb.at[0, w, rows], gb.at[1, w, rows], d2s.at[w], d2r.at[w], sib)

    def d2d(w, src=None):
        return remote(gb.at[0, w] if src is None else src, gb.at[1, w], d2s.at[w], d2r.at[w], sib)

    def pump(v, q):
        for d in range(2):
            @pl.when(goes(v, d, q))
            def _():
                ag_copy(v, d, q).wait_recv()

                @pl.when((v % G < G - 1) & goes(v + 1, d, q))
                def _():
                    ag_copy(v + 1, d, q).start()

                d2d_part(land(v, d), q).start()

        @pl.when((v == G - 2) & (q == SUB - 1))
        def _():
            for p in range(SUB):
                for d in range(2):
                    ag_copy(G, d, p).start()

    bar = pltpu.get_barrier_semaphore()
    for dev in (*nxt, sib):
        pl.semaphore_signal(bar, inc=1, device_id={"tp": dev}, device_id_type=MESH)
    pl.semaphore_wait(bar, 3)
    for q in range(SUB):
        for d in range(2):
            ag_copy(0, d, q, dy).start()
    d2d(S - 1, dy).start()
    d2d(2 * S - 1, x).start()

    def first(hT):
        def p1(w1, a, prb, wst):
            load_w1 = pltpu.make_async_copy(w_down, w1, wsem.at[0])
            own = [pltpu.make_async_copy(src, a.at[0, i], lsem.at[i]) for i, src in enumerate((dy, x))]
            put = [pltpu.make_async_copy(a.at[0, i], gb.at[0, (i + 1) * S - 1], lsem.at[i]) for i in range(2)]
            for c in own:
                c.start()
            load_w1.start()
            for o, c in zip(own, put):
                o.wait()
                c.start()
            for c in put:
                c.wait()

            def slot_of(u):
                return (u + S - 1) % S

            def loads(u):
                e, b = slot_of(u), u % 2
                out = [pltpu.make_async_copy(gb.at[:, e], a.at[b], lsem.at[b])]
                away = jnp.where(e == S - 1, 0, jnp.where(e == S - 2, S // 2, jnp.where(e % 2 == 0, S - 1 - e // 2, e // 2 + 1)))
                for h, (ps, cr) in enumerate(((pos, core), (pos2, 1 - core))):
                    row = pl.multiple_of((ring_chip(side, ps + away - S, cr) * 2 + cr) * R, R)
                    out.append(pltpu.make_async_copy(pre.at[pl.ds(row, R)], prb.at[b, h], psem.at[b, h]))
                rows = pl.ds(pl.multiple_of(u * (D // S), D // S), D // S)
                out.append(pltpu.make_async_copy(w_in.at[rows], wst, wsem.at[1]))
                return out

            def fetch(u):
                d2d(slot_of(u)).wait_recv()
                for c in loads(u):
                    c.start()

            fetch(0)
            load_w1.wait()

            @pl.loop(0, G + 1)
            def _(v):
                @pl.loop(0, 2)
                def _(half):
                    u = 2 * v - 1 + half
                    busy = (u >= 0) & (u < S) & ((v > 0) | (half == 1))

                    @pl.loop(0, SUB)
                    def _(j):
                        @pl.when(j % 2 == 0)
                        def _():
                            pump(v, half * (SUB // 2) + j // 2)

                        @pl.when(busy)
                        def _():
                            b = u % 2

                            @pl.when(j == 0)
                            def _():
                                for c in loads(u):
                                    c.wait()

                                w2[:, pl.ds(pl.multiple_of(u * (D // S), D // S), D // S)] = wst[...].T

                                @pl.when((half == 0) & (u + 1 < S))
                                def _():
                                    fetch(u + 1)

                            cols = pl.ds(pl.multiple_of(j * FC, FC), FC)
                            dh = dot(a[b].reshape(2 * R, D), w1[cols, :], 1, 1)
                            for h in range(2):
                                hid, slope = gelu_and_slope(prb[b, h, :, cols].astype(F32))
                                dpre[h, slot_of(u), :, cols] = (dh[h * R : (h + 1) * R] * slope).astype(BF16)
                                tok = pl.ds(pl.multiple_of((h * S + slot_of(u)) * R, R), R)
                                hT[cols, tok] = hid.T.astype(BF16)

                            @pl.when((j == SUB - 1) & (half == 1) & (u + 1 < S))
                            def _():
                                fetch(u + 1)

        pl.run_scoped(p1, pltpu.VMEM((F, D), BF16), pltpu.VMEM((2, 2, R, D), BF16), pltpu.VMEM((2, 2, R, F), BF16),
                      pltpu.VMEM((D // S, F), BF16))

        def p2(tile, dout, sst):
            def tile_load(i):
                cols = pl.ds(pl.multiple_of(i * TILE, TILE), TILE)
                return pltpu.make_async_copy(gb.at[:, pl.ds(0, S), :, cols], tile.at[i % 2], tsem.at[i % 2])

            def tile_out(i):
                cols = pl.ds(pl.multiple_of(i * TILE, TILE), TILE)
                return pltpu.make_async_copy(dout.at[i % 2], dw_down.at[:, cols], osem.at[i % 2])

            def sib_copy(k, c):
                return remote(sst.at[k % 2, c], sbb.at[k, c], sbs.at[k % 2, c], sbr.at[k, c], sib)

            tile_load(0).start()

            @pl.loop(0, S)
            def _(g):
                def step(w):
                    @pl.when(w % 2 == 0)
                    def _():
                        pump(G + 1 + w // (2 * SUB), (w // 2) % SUB)

                @pl.loop(0, 2)
                def _(j):
                    step(3 * g + j)
                    i = 2 * g + j
                    tile_load(i).wait()

                    @pl.when(i + 1 < NT)
                    def _():
                        tile_load(i + 1).start()

                    @pl.when(i >= 2)
                    def _():
                        tile_out(i - 2).wait()

                    dout[i % 2] = dot(hT[...], tile[i % 2].reshape(2 * S * R, TILE), 1, 0).astype(BF16)
                    tile_out(i).start()

                step(3 * g + 2)

                @pl.loop(0, 2)
                def _(j):
                    k, c = G - 1 - g // 2, (g % 2) * 2 + j

                    @pl.when(g >= 4)
                    def _():
                        sib_copy(k + 2, c).wait_send()

                    part = dot(dpre[1, pl.ds(2 * k, 2)].reshape(2 * R, F), w2[:, pl.ds(pl.multiple_of(c * DC, DC), DC)], 1, 0)
                    sst[k % 2, c] = part.astype(BF16).reshape(2, R, DC)
                    sib_copy(k, c).start()

            for i in range(NT - 2, NT):
                tile_out(i).wait()

            for k in range(2):
                for c in range(SUB):
                    sib_copy(k, c).wait_send()

        pl.run_scoped(p2, pltpu.VMEM((2, 2, S, R, TILE), BF16), pltpu.VMEM((2, F, TILE), BF16), pltpu.VMEM((2, SUB, 2, R, DC), BF16))

    pl.run_scoped(first, pltpu.VMEM((F, 2 * S * R), BF16))

    def p3(own, xt, eo, got, gsib, out, tb):
        def x_load(i):
            cols = pl.ds(pl.multiple_of(i * TILE, TILE), TILE)
            return pltpu.make_async_copy(gb.at[:, pl.ds(S, S), :, cols], xt.at[i % 2], tsem.at[i % 2])

        def e_out(i):
            return pltpu.make_async_copy(eo.at[i % 2], dw_in.at[pl.ds(pl.multiple_of(i * TILE, TILE), TILE)], osem.at[i % 2])

        def rs_copy(r, i, q):
            return remote(out.at[r % 2, q, i], rsb.at[r, q, i], rss.at[r % 2, i, q], rsr.at[r, i, q], nxt[1 - i])

        def rs_half(i, q):
            rows = pl.ds(H * (1 - i), H)
            return remote(out.at[0, q, 0, rows], rsb.at[0, q, i, rows], rss.at[0, i, q], rsr.at[0, i, q], nxt[1 - i])

        def got_load(r, q):
            return pltpu.make_async_copy(rsb.at[r - 1, q], got.at[q % 2], lsem.at[q % 2])

        def got_half(i, q):
            rows = pl.ds(H * (1 - i), H)
            return pltpu.make_async_copy(rsb.at[0, q, i, rows], got.at[q % 2, i, rows], fsem.at[2 + i, q])

        def sib_load(r, q):
            return pltpu.make_async_copy(sbb.at[G - 1 - r, q], gsib.at[q % 2], psem.at[0, q % 2])

        def sib_arrive(r, q):
            remote(sbb.at[G - 1 - r, q], sbb.at[G - 1 - r, q], sbs.at[0, q], sbr.at[G - 1 - r, q], sib).wait_recv()

        def col(q):
            return pl.ds(pl.multiple_of(q * DC, DC), DC)

        def snd_out(q):
            return [pltpu.make_async_copy(out.at[(G - 1) % 2, q, i], snd.at[:, col(q)], fsem.at[i, q]) for i, snd in ((1, snd0), (0, snd1))]

        def term_out(q):
            return pltpu.make_async_copy(tb.at[q % 2], terms.at[:, col(q)], wsem.at[1 + q % 2])

        got[...] = jnp.zeros_like(got)
        sib_arrive(0, 0)
        sib_load(0, 0).start()

        @pl.loop(0, G)
        def _(r):
            @pl.loop(0, SUB)
            def _(q):
                k = G - 1 - r
                part = dot(dpre[0, pl.ds(2 * k, 2)].reshape(2 * R, F), w2[:, col(q)], 1, 0)
                own[...] = part.reshape(2, R, DC)
                sib_load(r, q).wait()

                @pl.when(r == 0)
                def _():
                    out[0, q, 0] = (own[0] + gsib[q % 2, 0].astype(F32)).astype(BF16)
                    for i in range(2):
                        rs_half(i, q).start()

                    @pl.when(q >= 2)
                    def _():
                        term_out(q - 2).wait()

                    tb[q % 2] = own[1] + gsib[q % 2, 1].astype(F32)
                    term_out(q).start()
                    pump(2 * G - 1, q)

                @pl.when(r == 2)
                def _():
                    for i in range(2):
                        rs_half(i, q).wait_send()

                @pl.when(r > 2)
                def _():
                    for i in range(2):
                        rs_copy(r - 2, i, q).wait_send()

                @pl.when(r == 1)
                def _():
                    for i in range(2):
                        got_half(i, q).wait()

                @pl.when(r > 1)
                def _():
                    got_load(r, q).wait()

                @pl.when(r > 0)
                def _():
                    out[r % 2, q] = (own[...] + gsib[q % 2].astype(F32) + got[q % 2].astype(F32)).astype(BF16)

                @pl.when((r > 0) & (r < G - 1))
                def _():
                    for i in range(2):
                        rs_copy(r, i, q).start()

                @pl.when(r == G - 1)
                def _():
                    for c in snd_out(q):
                        c.start()

                @pl.when((r < G - 1) | (q < SUB - 1))
                def _():
                    q1 = (q + 1) % SUB
                    r1 = r + (q + 1) // SUB
                    sib_arrive(r1, q1)
                    sib_load(r1, q1).start()

                    @pl.when(r1 == 1)
                    def _():
                        for i in range(2):
                            rs_half(i, q1).wait_recv()
                            got_half(i, q1).start()

                    @pl.when(r1 > 1)
                    def _():
                        for i in range(2):
                            rs_copy(r1 - 1, i, q1).wait_recv()
                        got_load(r1, q1).start()

                extra = jnp.where(r < G - 2, 1, 0)
                base = SUB * (r - 1) + jnp.minimum(r - 1, G - 3) + q + jnp.where(q > 0, extra, 0)
                count = jnp.where(q == 0, 1 + extra, 1)

                @pl.loop(0, jnp.where(r == 0, 0, jnp.minimum(count, NT - base)))
                def _(jj):
                    i = base + jj

                    @pl.when(i == 0)
                    def _():
                        @pl.loop(S, 2 * S)
                        def _(w):
                            d2d(w).wait_recv()

                        x_load(0).start()

                    x_load(i).wait()

                    @pl.when(i + 1 < NT)
                    def _():
                        x_load(i + 1).start()

                    @pl.when(i >= 2)
                    def _():
                        e_out(i - 2).wait()

                    eo[i % 2] = dot(xt[i % 2].reshape(2 * S * R, TILE), dpre[...].reshape(2 * S * R, F), 0, 0).astype(BF16)
                    e_out(i).start()

        for i in range(NT - 2, NT):
            e_out(i).wait()
        for q in range(SUB):
            for i in range(2):
                rs_copy(G - 2, i, q).wait_send()
            for c in snd_out(q):
                c.wait()
        for q in range(SUB - 2, SUB):
            term_out(q).wait()

    pl.run_scoped(p3, pltpu.VMEM((2, R, DC), F32), pltpu.VMEM((2, 2, S, R, TILE), BF16), pltpu.VMEM((2, TILE, F), BF16),
                  pltpu.VMEM((2, 2, R, DC), BF16), pltpu.VMEM((2, 2, R, DC), BF16), pltpu.VMEM((2, SUB, 2, R, DC), BF16),
                  pltpu.VMEM((2, R, DC), F32))

    @pl.loop(0, 2 * G)
    def _(v):
        for d in range(2):
            @pl.when(v % G < G - 1)
            def _():
                remote(gb.at[0, 0], gb.at[0, 0], ags.at[v, d], agr.at[v, d, 0], nxt[d]).wait_send()

            @pl.when(v % G == G - 1)
            def _():
                half = gb.at[0, 0, pl.ds(0, H)]
                remote(half, half, ags.at[v, d], agr.at[v, d, 0], nxt[d]).wait_send()

    @pl.loop(0, 2 * S)
    def _(w):
        d2d(w).wait_send()


def copy_kernel(src, dst, buf, isem, osem):
    parts = isem.shape[0]
    rows = src.shape[0] // parts
    get = [pltpu.make_async_copy(src.at[pl.ds(i * rows, rows)], buf.at[i], isem.at[i]) for i in range(parts)]
    put = [pltpu.make_async_copy(buf.at[i], dst.at[pl.ds(i * rows, rows)], osem.at[i]) for i in range(parts)]
    for c in get:
        c.start()
    for g, p in zip(get, put):
        g.wait()
        p.start()
    for c in put:
        c.wait()


def copied(a):
    parts = 16
    return pl.pallas_call(
        copy_kernel,
        out_shape=jax.ShapeDtypeStruct(a.shape, a.dtype),
        in_specs=[pl.BlockSpec(memory_space=pl.ANY)],
        out_specs=pl.BlockSpec(memory_space=pl.ANY),
        scratch_shapes=[pltpu.VMEM((parts, a.shape[0] // parts, a.shape[1]), a.dtype), pltpu.SemaphoreType.DMA((parts,)), pltpu.SemaphoreType.DMA((parts,))],
        compiler_params=pltpu.CompilerParams(vmem_limit_bytes=60 * 2**20),
        cost_estimate=pl.CostEstimate(flops=4 * 10**9, bytes_accessed=4 * a.size, transcendentals=0),
        name="copy_out",
    )(a)


def solution(mesh):
    n = mesh.shape["tp"]
    S = n // 2
    G = S // 2
    perms = ring_perms(n)

    def step(x, dy, pre, w_in, w_down):
        R, D = x.shape
        F = pre.shape[1]
        sds = jax.ShapeDtypeStruct
        dma = pltpu.SemaphoreType.DMA
        *sums, term, dw_in, dw_down, _, _, _ = pl.pallas_call(
            functools.partial(kernel, n),
            out_shape=(
                sds((R, D), BF16), sds((R, D), BF16), sds((R, D), F32), sds((D, F), BF16), sds((F, D), BF16),
                sds((2, 2 * S, R, D), BF16), sds((G - 1, SUB, 2, R, D // SUB), BF16), sds((G, SUB, 2, R, D // SUB), BF16),
            ),
            in_specs=[pl.BlockSpec(memory_space=pl.ANY)] * 5,
            out_specs=[pl.BlockSpec(memory_space=pl.ANY)] * 8,
            scratch_shapes=[
                pltpu.VMEM((2, S, R, F), BF16), pltpu.VMEM((F, D), BF16),
                dma((2 * G, 2, SUB)), dma((2 * G, 2)), dma((2 * S,)), dma((2 * S,)),
                dma((G - 1, 2, SUB)), dma((2, 2, SUB)), dma((G, SUB)), dma((2, SUB)),
                dma((3,)), dma((2, 2)), dma((2,)), dma((2,)), dma((2,)), dma((4, SUB)),
            ],
            compiler_params=pltpu.CompilerParams(collective_id=0, has_side_effects=True, vmem_limit_bytes=VMEM_LIMIT),
            name="mlp_backward",
        )(x, dy, pre, w_in, w_down)
        dw_in, dw_down = copied(dw_in), copied(dw_down)
        ahead, back = (lax.ppermute(a, "tp", perm) for a, perm in zip(sums, perms))
        dx = (term + ahead.astype(F32) + back.astype(F32)).astype(BF16)
        return dx, dw_in, dw_down

    rows, cols = P(("dp", "tp"), None), P("dp", "tp")
    return jax.shard_map(
        step, mesh=mesh, in_specs=(rows, rows, cols, P(None, "tp"), P("tp", None)),
        out_specs=(rows, cols, rows), check_vma=False,
    )
```

```python
import functools
import math

import jax
import jax.numpy as jnp
from jax import lax
from jax.experimental import pallas as pl
from jax.experimental.pallas import tpu as pltpu
from jax.sharding import PartitionSpec as P

MESH = pl.DeviceIdType.MESH
F32, BF16 = jnp.float32, jnp.bfloat16
SUB = 4
TILE = 256
VMEM_LIMIT = 63 * 2**20


def ring_pos(side, chip, ring):
    a, b = chip // side, chip % side
    return jnp.where(ring == 0, a, b) * side + (a + b) % side


def ring_chip(side, pos, ring):
    pos = (pos + side * side) % (side * side)
    major = pos // side
    minor = (pos % side - major + side) % side
    return jnp.where(ring == 0, major * side + minor, minor * side + major)


def ring_perms(n):
    S = n // 2
    side = math.isqrt(S)
    with jax.ensure_compile_time_eval():
        ring = [[int(ring_chip(side, p, c)) * 2 + c for p in range(S)] for c in range(2)]
    return [[(r[p], r[(p + d) % S]) for r in ring for p in range(S)] for d in (1, -1)]


def dot(a, b, ca, cb):
    return lax.dot_general(a, b, (((ca,), (cb,)), ((), ())), preferred_element_type=F32)


def gelu_and_slope(p):
    c = math.sqrt(2.0 / math.pi)
    sq = p * p
    t = jnp.tanh(c * (p + 0.044715 * (sq * p)))
    cdf = 0.5 * (1.0 + t)
    slope = cdf + p * (0.5 * (1.0 - t * t)) * (c * (1.0 + 3 * 0.044715 * sq))
    return p * cdf, slope


def kernel(n, x, dy, pre, w_in, w_down, snd0, snd1, terms, dw_in, dw_down, gb, rsb, sbb, dpre, w2,
           agr, ags, d2r, d2s, rsr, rss, sbr, sbs, wsem, psem, osem, lsem, tsem, fsem):
    S = n // 2
    G = S // 2
    side = math.isqrt(S)
    R, D = x.shape
    H, Q, F = R // 2, R // SUB, pre.shape[1]
    DC, FC = D // SUB, F // SUB
    NT = D // TILE
    me = lax.axis_index("tp")
    chip, core = me // 2, me % 2
    pos, pos2 = ring_pos(side, chip, core), ring_pos(side, chip, 1 - core)
    nxt = [ring_chip(side, pos + 1, core) * 2 + core, ring_chip(side, pos - 1, core) * 2 + core]
    sib = chip * 2 + 1 - core

    def remote(src, dst, ssem, rsem, dev):
        return pltpu.make_async_remote_copy(src, dst, ssem, rsem, device_id={"tp": dev}, device_id_type=MESH)

    def land(v, d):
        return S * (v // G) + jnp.where(v % G == G - 1, S - 2, 2 * (v % G) + d)

    def ag_copy(v, d, q, src=None):
        rows = pl.ds(q * Q if isinstance(q, int) else pl.multiple_of(q * Q, Q), Q)
        slot = S * (v // G) + jnp.where(v % G == 0, S - 1, 2 * (v % G - 1) + d)
        src = gb.at[0, slot, rows] if src is None else src.at[rows]
        return remote(src, gb.at[0, land(v, d), rows], ags.at[v, d], agr.at[v, d, q], nxt[d])

    def goes(v, d, q):
        return (v % G < G - 1) | ((q >= SUB // 2) if d else (q < SUB // 2))

    def d2d_part(w, q):
        rows = pl.ds(pl.multiple_of(q * Q, Q), Q)
        return remote(gb.at[0, w, rows], gb.at[1, w, rows], d2s.at[w], d2r.at[w], sib)

    def d2d(w, src=None):
        return remote(gb.at[0, w] if src is None else src, gb.at[1, w], d2s.at[w], d2r.at[w], sib)

    def pump(v, q):
        for d in range(2):
            @pl.when(goes(v, d, q))
            def _():
                ag_copy(v, d, q).wait_recv()

                @pl.when((v % G < G - 1) & goes(v + 1, d, q))
                def _():
                    ag_copy(v + 1, d, q).start()

                d2d_part(land(v, d), q).start()

        @pl.when((v == G - 2) & (q == SUB - 1))
        def _():
            for p in range(SUB):
                for d in range(2):
                    ag_copy(G, d, p).start()

    bar = pltpu.get_barrier_semaphore()
    for dev in (*nxt, sib):
        pl.semaphore_signal(bar, inc=1, device_id={"tp": dev}, device_id_type=MESH)
    pl.semaphore_wait(bar, 3)
    for q in range(SUB):
        for d in range(2):
            ag_copy(0, d, q, dy).start()
    d2d(S - 1, dy).start()
    d2d(2 * S - 1, x).start()

    def first(hT):
        def p1(w1, a, prb, wst):
            load_w1 = pltpu.make_async_copy(w_down, w1, wsem.at[0])
            own = [pltpu.make_async_copy(src, a.at[0, i], lsem.at[i]) for i, src in enumerate((dy, x))]
            put = [pltpu.make_async_copy(a.at[0, i], gb.at[0, (i + 1) * S - 1], lsem.at[i]) for i in range(2)]
            for c in own:
                c.start()
            load_w1.start()
            for o, c in zip(own, put):
                o.wait()
                c.start()
            for c in put:
                c.wait()

            def slot_of(u):
                return (u + S - 1) % S

            def loads(u):
                e, b = slot_of(u), u % 2
                out = [pltpu.make_async_copy(gb.at[:, e], a.at[b], lsem.at[b])]
                away = jnp.where(e == S - 1, 0, jnp.where(e == S - 2, S // 2, jnp.where(e % 2 == 0, S - 1 - e // 2, e // 2 + 1)))
                for h, (ps, cr) in enumerate(((pos, core), (pos2, 1 - core))):
                    row = pl.multiple_of((ring_chip(side, ps + away - S, cr) * 2 + cr) * R, R)
                    out.append(pltpu.make_async_copy(pre.at[pl.ds(row, R)], prb.at[b, h], psem.at[b, h]))
                rows = pl.ds(pl.multiple_of(u * (D // S), D // S), D // S)
                out.append(pltpu.make_async_copy(w_in.at[rows], wst, wsem.at[1]))
                return out

            def fetch(u):
                d2d(slot_of(u)).wait_recv()
                for c in loads(u):
                    c.start()

            fetch(0)
            load_w1.wait()

            @pl.loop(0, G + 1)
            def _(v):
                @pl.loop(0, 2)
                def _(half):
                    u = 2 * v - 1 + half
                    busy = (u >= 0) & (u < S) & ((v > 0) | (half == 1))

                    @pl.loop(0, SUB)
                    def _(j):
                        @pl.when(j % 2 == 0)
                        def _():
                            pump(v, half * (SUB // 2) + j // 2)

                        @pl.when(busy)
                        def _():
                            b = u % 2

                            @pl.when(j == 0)
                            def _():
                                for c in loads(u):
                                    c.wait()

                                w2[:, pl.ds(pl.multiple_of(u * (D // S), D // S), D // S)] = wst[...].T

                                @pl.when((half == 0) & (u + 1 < S))
                                def _():
                                    fetch(u + 1)

                            cols = pl.ds(pl.multiple_of(j * FC, FC), FC)
                            dh = dot(a[b].reshape(2 * R, D), w1[cols, :], 1, 1)
                            for h in range(2):
                                hid, slope = gelu_and_slope(prb[b, h, :, cols].astype(F32))
                                dpre[h, slot_of(u), :, cols] = (dh[h * R : (h + 1) * R] * slope).astype(BF16)
                                tok = pl.ds(pl.multiple_of((h * S + slot_of(u)) * R, R), R)
                                hT[cols, tok] = hid.T.astype(BF16)

                            @pl.when((j == SUB - 1) & (half == 1) & (u + 1 < S))
                            def _():
                                fetch(u + 1)

        pl.run_scoped(p1, pltpu.VMEM((F, D), BF16), pltpu.VMEM((2, 2, R, D), BF16), pltpu.VMEM((2, 2, R, F), BF16),
                      pltpu.VMEM((D // S, F), BF16))

        def p2(tile, dout, sst):
            def tile_load(i):
                cols = pl.ds(pl.multiple_of(i * TILE, TILE), TILE)
                return pltpu.make_async_copy(gb.at[:, pl.ds(0, S), :, cols], tile.at[i % 2], tsem.at[i % 2])

            def tile_out(i):
                cols = pl.ds(pl.multiple_of(i * TILE, TILE), TILE)
                return pltpu.make_async_copy(dout.at[i % 2], dw_down.at[:, cols], osem.at[i % 2])

            def sib_copy(k, c):
                return remote(sst.at[k % 2, c], sbb.at[k, c], sbs.at[k % 2, c], sbr.at[k, c], sib)

            tile_load(0).start()

            @pl.loop(0, S)
            def _(g):
                def step(w):
                    @pl.when(w % 2 == 0)
                    def _():
                        pump(G + 1 + w // (2 * SUB), (w // 2) % SUB)

                step(3 * g)

                @pl.loop(0, 2)
                def _(j):
                    k, c = G - 1 - g // 2, (g % 2) * 2 + j

                    @pl.when(g >= 4)
                    def _():
                        sib_copy(k + 2, c).wait_send()

                    part = dot(dpre[1, pl.ds(2 * k, 2)].reshape(2 * R, F), w2[:, pl.ds(pl.multiple_of(c * DC, DC), DC)], 1, 0)
                    sst[k % 2, c] = part.astype(BF16).reshape(2, R, DC)
                    sib_copy(k, c).start()

                @pl.loop(0, 2)
                def _(j):
                    step(3 * g + 1 + j)
                    i = 2 * g + j
                    tile_load(i).wait()

                    @pl.when(i + 1 < NT)
                    def _():
                        tile_load(i + 1).start()

                    @pl.when(i >= 2)
                    def _():
                        tile_out(i - 2).wait()

                    dout[i % 2] = dot(hT[...], tile[i % 2].reshape(2 * S * R, TILE), 1, 0).astype(BF16)
                    tile_out(i).start()

            for i in range(NT - 2, NT):
                tile_out(i).wait()

            for k in range(2):
                for c in range(SUB):
                    sib_copy(k, c).wait_send()

        pl.run_scoped(p2, pltpu.VMEM((2, 2, S, R, TILE), BF16), pltpu.VMEM((2, F, TILE), BF16), pltpu.VMEM((2, SUB, 2, R, DC), BF16))

    pl.run_scoped(first, pltpu.VMEM((F, 2 * S * R), BF16))

    def sent():
        @pl.loop(0, 2 * G)
        def _(v):
            for d in range(2):
                @pl.when(v % G < G - 1)
                def _():
                    remote(gb.at[0, 0], gb.at[0, 0], ags.at[v, d], agr.at[v, d, 0], nxt[d]).wait_send()

                @pl.when(v % G == G - 1)
                def _():
                    half = gb.at[0, 0, pl.ds(0, H)]
                    remote(half, half, ags.at[v, d], agr.at[v, d, 0], nxt[d]).wait_send()

        @pl.loop(0, 2 * S)
        def _(w):
            d2d(w).wait_send()

    def p3(own, xt, eo, got, gsib, out, tb):
        def x_load(i):
            cols = pl.ds(pl.multiple_of(i * TILE, TILE), TILE)
            return pltpu.make_async_copy(gb.at[:, pl.ds(S, S), :, cols], xt.at[i % 2], tsem.at[i % 2])

        def e_out(i):
            return pltpu.make_async_copy(eo.at[i % 2], dw_in.at[pl.ds(pl.multiple_of(i * TILE, TILE), TILE)], osem.at[i % 2])

        def rs_copy(r, i, q):
            return remote(out.at[r % 2, q, i], rsb.at[r, q, i], rss.at[r % 2, i, q], rsr.at[r, i, q], nxt[1 - i])

        def rs_half(i, q):
            rows = pl.ds(H * (1 - i), H)
            return remote(out.at[0, q, 0, rows], rsb.at[0, q, i, rows], rss.at[0, i, q], rsr.at[0, i, q], nxt[1 - i])

        def got_load(r, i, q):
            return pltpu.make_async_copy(rsb.at[r - 1, q, i], got.at[q % 2, i], fsem.at[2 + i, q])

        def got_half(i, q):
            rows = pl.ds(H * (1 - i), H)
            return pltpu.make_async_copy(rsb.at[0, q, i, rows], got.at[q % 2, i, rows], fsem.at[2 + i, q])

        def sib_load(r, q):
            return pltpu.make_async_copy(sbb.at[G - 1 - r, q], gsib.at[q % 2], psem.at[0, q % 2])

        def sib_arrive(r, q):
            remote(sbb.at[G - 1 - r, q], sbb.at[G - 1 - r, q], sbs.at[0, q], sbr.at[G - 1 - r, q], sib).wait_recv()

        def col(q):
            return pl.ds(pl.multiple_of(q * DC, DC), DC)

        def snd_out(i, q):
            return pltpu.make_async_copy(out.at[(G - 1) % 2, q, i], (snd1, snd0)[i].at[:, col(q)], fsem.at[i, q])

        def term_out(q):
            return pltpu.make_async_copy(tb.at[q % 2], terms.at[:, col(q)], wsem.at[1 + q % 2])

        def own_terms(r, q):
            k = G - 1 - r
            part = dot(dpre[0, pl.ds(2 * k, 2)].reshape(2 * R, F), w2[:, col(q)], 1, 0)
            own[...] = part.reshape(2, R, DC)

        sib_arrive(0, 0)
        sib_load(0, 0).start()
        own_terms(0, 0)

        @pl.loop(0, G)
        def _(r):
            @pl.loop(0, SUB)
            def _(q):
                @pl.when((r == 0) & (q == 0))
                def _():
                    got[...] = jnp.zeros_like(got)

                sib_load(r, q).wait()

                @pl.when(r == 0)
                def _():
                    out[0, q, 0] = (own[0] + gsib[q % 2, 0].astype(F32)).astype(BF16)
                    for i in range(2):
                        rs_half(i, q).start()

                    @pl.when(q >= 2)
                    def _():
                        term_out(q - 2).wait()

                    tb[q % 2] = own[1] + gsib[q % 2, 1].astype(F32)
                    term_out(q).start()
                    pump(2 * G - 1, q)

                @pl.when(r == 2)
                def _():
                    for i in range(2):
                        rs_half(i, q).wait_send()

                for i in range(2):
                    @pl.when(r > 2)
                    def _():
                        rs_copy(r - 2, i, q).wait_send()

                    @pl.when(r == 1)
                    def _():
                        got_half(i, q).wait()

                    @pl.when(r > 1)
                    def _():
                        got_load(r, i, q).wait()

                    @pl.when(r > 0)
                    def _():
                        out[r % 2, q, i] = (own[i] + gsib[q % 2, i].astype(F32) + got[q % 2, i].astype(F32)).astype(BF16)

                    @pl.when((r > 0) & (r < G - 1))
                    def _():
                        rs_copy(r, i, q).start()

                    @pl.when(r == G - 1)
                    def _():
                        snd_out(i, q).start()

                @pl.when((r < G - 1) | (q < SUB - 1))
                def _():
                    q1 = (q + 1) % SUB
                    r1 = r + (q + 1) // SUB
                    sib_arrive(r1, q1)
                    sib_load(r1, q1).start()
                    own_terms(r1, q1)

                    @pl.when(r1 == 1)
                    def _():
                        for i in range(2):
                            rs_half(i, q1).wait_recv()
                            got_half(i, q1).start()

                    @pl.when(r1 > 1)
                    def _():
                        for i in range(2):
                            rs_copy(r1 - 1, i, q1).wait_recv()
                            got_load(r1, i, q1).start()

                extra = jnp.where(r < G - 1, 1, 0)
                base = (SUB + 1) * (r - 1) + q + jnp.where(q > 0, extra, 0)
                count = jnp.where(q == 0, 1 + extra, 1)

                @pl.loop(0, jnp.where(r == 0, 0, jnp.minimum(count, NT - base)))
                def _(jj):
                    i = base + jj

                    @pl.when(i == 0)
                    def _():
                        @pl.loop(S, 2 * S)
                        def _(w):
                            d2d(w).wait_recv()

                        x_load(0).start()

                    x_load(i).wait()

                    @pl.when(i == NT // 2)
                    def _():
                        sent()

                    @pl.when(i + 1 < NT)
                    def _():
                        x_load(i + 1).start()

                    @pl.when(i >= 2)
                    def _():
                        e_out(i - 2).wait()

                    eo[i % 2] = dot(xt[i % 2].reshape(2 * S * R, TILE), dpre[...].reshape(2 * S * R, F), 0, 0).astype(BF16)
                    e_out(i).start()

        for i in range(NT - 2, NT):
            e_out(i).wait()
        for q in range(SUB):
            for i in range(2):
                rs_copy(G - 2, i, q).wait_send()
            for i in range(2):
                snd_out(i, q).wait()
        for q in range(SUB - 2, SUB):
            term_out(q).wait()

    pl.run_scoped(p3, pltpu.VMEM((2, R, DC), F32), pltpu.VMEM((2, 2, S, R, TILE), BF16), pltpu.VMEM((2, TILE, F), BF16),
                  pltpu.VMEM((2, 2, R, DC), BF16), pltpu.VMEM((2, 2, R, DC), BF16), pltpu.VMEM((2, SUB, 2, R, DC), BF16),
                  pltpu.VMEM((2, R, DC), F32))


def copy_kernel(a, b, a2, b2, abuf, bbuf, isem, osem):
    get, put = [], []
    for src, dst, buf in ((a, a2, abuf), (b, b2, bbuf)):
        parts, rows = buf.shape[:2]
        for i in range(parts):
            at = pl.ds(i * rows, rows)
            get.append(pltpu.make_async_copy(src.at[at], buf.at[i], isem.at[len(get)]))
            put.append(pltpu.make_async_copy(buf.at[i], dst.at[at], osem.at[len(put)]))
    for c in get:
        c.start()
    for g, p in zip(get, put):
        g.wait()
        p.start()
    for c in put:
        c.wait()


def copied(a, b):
    parts = 4
    dma = pltpu.SemaphoreType.DMA
    return pl.pallas_call(
        copy_kernel,
        out_shape=[jax.ShapeDtypeStruct(t.shape, t.dtype) for t in (a, b)],
        in_specs=[pl.BlockSpec(memory_space=pl.ANY)] * 2,
        out_specs=[pl.BlockSpec(memory_space=pl.ANY)] * 2,
        scratch_shapes=[pltpu.VMEM((parts, t.shape[0] // parts, t.shape[1]), t.dtype) for t in (a, b)] + [dma((2 * parts,))] * 2,
        compiler_params=pltpu.CompilerParams(vmem_limit_bytes=48 * 2**20),
        cost_estimate=pl.CostEstimate(flops=8 * 10**9, bytes_accessed=8 * a.size, transcendentals=0),
        name="copy_out",
    )(a, b)


def add_kernel(a, b, c, o):
    o[...] = (a[...] + b[...].astype(F32) + c[...].astype(F32)).astype(BF16)


def added(term, ahead, back):
    whole = pl.BlockSpec(memory_space=pltpu.VMEM)
    return pl.pallas_call(
        add_kernel, in_specs=[whole] * 3, out_specs=whole, out_shape=jax.ShapeDtypeStruct(term.shape, BF16), name="last_add",
        compiler_params=pltpu.CompilerParams(vmem_limit_bytes=16 * 2**20),
    )(term, ahead, back)


def solution(mesh):
    n = mesh.shape["tp"]
    S = n // 2
    G = S // 2
    perms = ring_perms(n)

    def step(x, dy, pre, w_in, w_down):
        R, D = x.shape
        F = pre.shape[1]
        sds = jax.ShapeDtypeStruct
        dma = pltpu.SemaphoreType.DMA
        *sums, term, dw_in, dw_down, _, _, _ = pl.pallas_call(
            functools.partial(kernel, n),
            out_shape=(
                sds((R, D), BF16), sds((R, D), BF16), sds((R, D), F32), sds((D, F), BF16), sds((F, D), BF16),
                sds((2, 2 * S, R, D), BF16), sds((G - 1, SUB, 2, R, D // SUB), BF16), sds((G, SUB, 2, R, D // SUB), BF16),
            ),
            in_specs=[pl.BlockSpec(memory_space=pl.ANY)] * 5,
            out_specs=[pl.BlockSpec(memory_space=pl.ANY)] * 8,
            scratch_shapes=[
                pltpu.VMEM((2, S, R, F), BF16), pltpu.VMEM((F, D), BF16),
                dma((2 * G, 2, SUB)), dma((2 * G, 2)), dma((2 * S,)), dma((2 * S,)),
                dma((G - 1, 2, SUB)), dma((2, 2, SUB)), dma((G, SUB)), dma((2, SUB)),
                dma((3,)), dma((2, 2)), dma((2,)), dma((2,)), dma((2,)), dma((4, SUB)),
            ],
            compiler_params=pltpu.CompilerParams(collective_id=0, has_side_effects=True, vmem_limit_bytes=VMEM_LIMIT),
            name="mlp_backward",
        )(x, dy, pre, w_in, w_down)
        dw_in, dw_down = copied(dw_in, dw_down)
        ahead, back = (lax.ppermute(a, "tp", perm) for a, perm in zip(sums, perms))
        return added(term, ahead, back), dw_in, dw_down

    rows, cols = P(("dp", "tp"), None), P("dp", "tp")
    return jax.shard_map(
        step, mesh=mesh, in_specs=(rows, rows, cols, P(None, "tp"), P("tp", None)),
        out_specs=(rows, cols, rows), check_vma=False,
    )
```

```python
import functools
import math

import jax
import jax.numpy as jnp
from jax import lax
from jax.experimental import pallas as pl
from jax.experimental.pallas import tpu as pltpu
from jax.sharding import PartitionSpec as P

MESH = pl.DeviceIdType.MESH
F32, BF16 = jnp.float32, jnp.bfloat16
SUB = 4
TILE = 256
FILL = 512
VMEM_LIMIT = 67043328


def ring_pos(side, chip, ring):
    a, b = chip // side, chip % side
    return jnp.where(ring == 0, a, b) * side + (a + b) % side


def ring_chip(side, pos, ring):
    pos = (pos + side * side) % (side * side)
    major = pos // side
    minor = (pos % side - major + side) % side
    return jnp.where(ring == 0, major * side + minor, minor * side + major)


def ring_perms(n):
    S = n // 2
    side = math.isqrt(S)
    with jax.ensure_compile_time_eval():
        ring = [[int(ring_chip(side, p, c)) * 2 + c for p in range(S)] for c in range(2)]
    return [[(r[p], r[(p + d) % S]) for r in ring for p in range(S)] for d in (1, -1)]


def dot(a, b, ca, cb):
    return lax.dot_general(a, b, (((ca,), (cb,)), ((), ())), preferred_element_type=F32)


def gelu_and_slope(p):
    c = math.sqrt(2.0 / math.pi)
    sq = p * p
    t = jnp.tanh(c * (p + 0.044715 * (sq * p)))
    cdf = 0.5 * (1.0 + t)
    slope = cdf + p * (0.5 * (1.0 - t * t)) * (c * (1.0 + 3 * 0.044715 * sq))
    return p * cdf, slope


def kernel(n, x, dy, pre, w_in, w_down, snd0, snd1, terms, filled, dw_in, dw_down, gb, rsb, sbb, dpre, w2, late,
           agr, ags, d2r, d2s, rsr, rss, sbr, sbs, wsem, psem, osem, lsem, tsem, fsem, gsem, xsem):
    S = n // 2
    G = S // 2
    side = math.isqrt(S)
    R, D = x.shape
    H, F = R // 2, pre.shape[1]
    DC, FC = D // SUB, F // SUB
    NT = D // TILE
    me = lax.axis_index("tp")
    chip, core = me // 2, me % 2
    pos, pos2 = ring_pos(side, chip, core), ring_pos(side, chip, 1 - core)
    nxt = [ring_chip(side, pos + 1, core) * 2 + core, ring_chip(side, pos - 1, core) * 2 + core]
    sib = chip * 2 + 1 - core

    def remote(src, dst, ssem, rsem, dev):
        return pltpu.make_async_remote_copy(src, dst, ssem, rsem, device_id={"tp": dev}, device_id_type=MESH)

    def arrived(ref, sem):
        remote(ref, ref, rss.at[0, 0], sem, sib).wait_recv()

    def left(ref, sem):
        remote(ref, ref, sem, rsr.at[0, 0], sib).wait_send()

    def land(v, d):
        return S * (v // G) + jnp.where(v % G == G - 1, S - 2, 2 * (v % G) + d)

    def half_of(e, d):
        q = (e + d) % 2
        return pl.ds(q * H if isinstance(q, int) else pl.multiple_of(q * H, H), H)

    def ag_copy(v, d, e, src=None):
        rows = half_of(e, d)
        slot = S * (v // G) + jnp.where(v % G == 0, S - 1, 2 * (v % G - 1) + d)
        src = gb.at[0, slot, rows] if src is None else src.at[rows]
        return remote(src, gb.at[0, land(v, d), rows], ags.at[v // (G // 2)], agr.at[v, e], nxt[d])

    def handed(w):
        return jnp.where(w < S - 2, w // 2, jnp.where(w < S, w - S // 2 + 1, S // 2 + 1 + (w - S) // (S // 2)))

    def hand(w, rows=None, src=None):
        ref = gb.at[0, w] if src is None else src
        dst = gb.at[1, w]
        if rows is not None:
            ref, dst = ref.at[rows], dst.at[rows]
        return remote(ref, dst, d2s.at[w // (S // 2)], d2r.at[handed(w)], sib)

    def pump(v, e):
        @pl.when((v % G < G - 1) | (e == 0))
        def _():
            arrived(gb.at[0, 0], agr.at[v, e])

            @pl.when((v % G < G - 2) | ((v % G == G - 2) & (e == 0)))
            def _():
                for d in range(2):
                    ag_copy(v + 1, d, e).start()

            @pl.when((v == G - 2) & (e == 1))
            def _():
                for p in range(2):
                    for d in range(2):
                        ag_copy(G, d, p).start()

            for d in range(2):
                hand(land(v, d), half_of(e, d)).start()

    bar = pltpu.get_barrier_semaphore()
    for dev in (*nxt, sib):
        pl.semaphore_signal(bar, inc=1, device_id={"tp": dev}, device_id_type=MESH)
    pl.semaphore_wait(bar, 3)
    for e in range(2):
        for d in range(2):
            ag_copy(0, d, e, dy).start()
    hand(S - 1, src=dy).start()
    hand(2 * S - 1, src=x).start()

    def first(hT):
        def p1(w1, a, prb, wst):
            load_w1 = pltpu.make_async_copy(w_down, w1, wsem.at[0])
            own = [pltpu.make_async_copy(src, a.at[0, i], lsem.at[i]) for i, src in enumerate((dy, x))]
            put = [pltpu.make_async_copy(a.at[0, i], gb.at[0, (i + 1) * S - 1], lsem.at[i]) for i in range(2)]
            for c in own:
                c.start()
            load_w1.start()
            for o, c in zip(own, put):
                o.wait()
                c.start()
            for c in put:
                c.wait()

            def slot_of(u):
                return (u + S - 1) % S

            def loads(u):
                e, b = slot_of(u), u % 2
                out = [pltpu.make_async_copy(gb.at[:, e], a.at[b], lsem.at[b])]
                away = jnp.where(e == S - 1, 0, jnp.where(e == S - 2, S // 2, jnp.where(e % 2 == 0, S - 1 - e // 2, e // 2 + 1)))
                for h, (ps, cr) in enumerate(((pos, core), (pos2, 1 - core))):
                    row = pl.multiple_of((ring_chip(side, ps + away - S, cr) * 2 + cr) * R, R)
                    out.append(pltpu.make_async_copy(pre.at[pl.ds(row, R)], prb.at[b, h], psem.at[b]))
                rows = pl.ds(pl.multiple_of(u * (D // S), D // S), D // S)
                out.append(pltpu.make_async_copy(w_in.at[rows], wst, wsem.at[1]))
                return out

            def fetch(u):
                @pl.when((u % 2 == 1) & (u < S - 1))
                def _():
                    arrived(gb.at[1, pl.ds(0, 2)], d2r.at[handed(slot_of(u))])

                @pl.when((u == 0) | (u == S - 1))
                def _():
                    arrived(gb.at[1, 0], d2r.at[handed(slot_of(u))])

                for c in loads(u):
                    c.start()

            def fetched(u):
                b = u % 2
                for ref, sem in ((a.at[b], lsem.at[b]), (prb.at[b], psem.at[b]), (wst, wsem.at[1])):
                    pltpu.make_async_copy(ref, ref, sem).wait()

            fetch(0)
            load_w1.wait()

            @pl.loop(0, G + 1)
            def _(v):
                @pl.loop(0, 2)
                def _(half):
                    u = 2 * v - 1 + half
                    busy = (u >= 0) & (u < S) & ((v > 0) | (half == 1))

                    @pl.loop(0, SUB)
                    def _(j):
                        @pl.when(j == 0)
                        def _():
                            pump(v, half)

                        @pl.when(busy)
                        def _():
                            b = u % 2

                            @pl.when(j == 0)
                            def _():
                                fetched(u)
                                w2[:, pl.ds(pl.multiple_of(u * (D // S), D // S), D // S)] = wst[...].T

                                @pl.when((half == 0) & (u + 1 < S))
                                def _():
                                    fetch(u + 1)

                            cols = pl.ds(pl.multiple_of(j * FC, FC), FC)
                            dh = dot(a[b].reshape(2 * R, D), w1[cols, :], 1, 1)
                            for h in range(2):
                                hid, slope = gelu_and_slope(prb[b, h, :, cols].astype(F32))
                                dpre[h, slot_of(u), :, cols] = (dh[h * R : (h + 1) * R] * slope).astype(BF16)
                                tok = pl.ds(pl.multiple_of((h * S + slot_of(u)) * R, R), R)
                                hT[cols, tok] = hid.T.astype(BF16)

                            @pl.when((j == SUB - 1) & (half == 1) & (u + 1 < S))
                            def _():
                                fetch(u + 1)

        pl.run_scoped(p1, pltpu.VMEM((F, D), BF16), pltpu.VMEM((2, 2, R, D), BF16), pltpu.VMEM((2, 2, R, F), BF16),
                      pltpu.VMEM((D // S, F), BF16))

        def p2(tile, dout, sst):
            def tile_load(i):
                cols = pl.ds(pl.multiple_of(i * TILE, TILE), TILE)
                return pltpu.make_async_copy(gb.at[:, pl.ds(0, S), :, cols], tile.at[i % 2], tsem.at[i % 2])

            def tile_out(i):
                cols = pl.ds(pl.multiple_of(i * TILE, TILE), TILE)
                return pltpu.make_async_copy(dout.at[i % 2], dw_down.at[:, cols], osem.at[i % 2])

            def sib_copy(k, c):
                return remote(sst.at[k % 2, c], sbb.at[k, c], sbs.at[k % 2], sbr.at[k], sib)

            tile_load(0).start()

            @pl.loop(0, S)
            def _(g):
                def step(w):
                    @pl.when(w % 4 == 3)
                    def _():
                        pump(G + 1 + w // 8, (w // 4) % 2)

                step(3 * g)

                @pl.loop(0, 2)
                def _(j):
                    k, c = G - 1 - g // 2, (g % 2) * 2 + j

                    @pl.when((g >= 4) & (c == 0))
                    def _():
                        left(sst.at[k % 2], sbs.at[k % 2])

                    part = dot(dpre[1, pl.ds(2 * k, 2)].reshape(2 * R, F), w2[:, pl.ds(pl.multiple_of(c * DC, DC), DC)], 1, 0)
                    sst[k % 2, c] = part.astype(BF16).reshape(2, R, DC)
                    sib_copy(k, c).start()

                @pl.loop(0, 2)
                def _(j):
                    step(3 * g + 1 + j)
                    i = 2 * g + j
                    tile_load(i).wait()

                    @pl.when(i + 1 < NT)
                    def _():
                        tile_load(i + 1).start()

                    @pl.when(i >= 2)
                    def _():
                        tile_out(i - 2).wait()

                    dout[i % 2] = dot(hT[...], tile[i % 2].reshape(2 * S * R, TILE), 1, 0).astype(BF16)
                    tile_out(i).start()

            for i in range(NT - 2, NT):
                tile_out(i).wait()

            for k in range(2):
                left(sst.at[k], sbs.at[k])

        pl.run_scoped(p2, pltpu.VMEM((2, 2, S, R, TILE), BF16), pltpu.VMEM((2, F, TILE), BF16), pltpu.VMEM((2, SUB, 2, R, DC), BF16))

    pl.run_scoped(first, pltpu.VMEM((F, 2 * S * R), BF16))

    def sent():
        for v in range(4):
            left(gb.at[0, pl.ds(0, S // 2 - v % 2)], ags.at[v])
            left(gb.at[0, pl.ds(0, S // 2)], d2s.at[v])

    def p3(own, xt, eo, got, gsib, out, tb):
        def x_load(i):
            cols = pl.ds(pl.multiple_of(i * TILE, TILE), TILE)
            return pltpu.make_async_copy(gb.at[:, pl.ds(S, S), :, cols], xt.at[i % 2], tsem.at[i % 2])

        def e_out(i):
            return pltpu.make_async_copy(eo.at[i % 2], dw_in.at[pl.ds(pl.multiple_of(i * TILE, TILE), TILE)], osem.at[i % 2])

        def rs_copy(r, i, q):
            return remote(out.at[r % 2, q, i], rsb.at[r, q, i], rss.at[r % 2, q], rsr.at[r, q], nxt[1 - i])

        def rs_late(i):
            r, q = G - 2, SUB - 1
            return remote(out.at[r % 2, q, i], late.at[i], rss.at[r % 2, q], rsr.at[r, q], nxt[1 - i])

        def rs_fill(i):
            return remote(out.at[(G - 1) % 2, 0, i, :, pl.ds(0, FILL)], filled.at[i], xsem.at[0], xsem.at[1], nxt[1 - i])

        def rs_half(i, q):
            rows = pl.ds(H * (1 - i), H)
            return remote(out.at[0, q, 0, rows], rsb.at[0, q, i, rows], rss.at[0, q], rsr.at[0, q], nxt[1 - i])

        def got_load(r, i, q):
            return pltpu.make_async_copy(rsb.at[r - 1, q, i], got.at[q % 2, i], gsem.at[q % 2, i])

        def got_half(i, q):
            rows = pl.ds(H * (1 - i), H)
            return pltpu.make_async_copy(rsb.at[0, q, i, rows], got.at[q % 2, i, rows], gsem.at[q % 2, i])

        def sib_load(r, q):
            return pltpu.make_async_copy(sbb.at[G - 1 - r, q], gsib.at[q % 2], psem.at[q % 2])

        def sib_arrive(r, q):
            @pl.when(q == 0)
            def _():
                arrived(sbb.at[G - 1 - r], sbr.at[G - 1 - r])

        def col(q):
            return pl.ds(pl.multiple_of(q * DC, DC), DC)

        def snd_out(i, q):
            if isinstance(q, int) and q == 0:
                cols, to = pl.ds(FILL, DC - FILL), pl.ds(0, DC - FILL)
            else:
                cols, to = pl.ds(0, DC), pl.ds(pl.multiple_of(q * DC - FILL, FILL), DC)
            return pltpu.make_async_copy(out.at[(G - 1) % 2, q, i, :, cols], (snd1, snd0)[i].at[:, to], fsem.at[i])

        def term_out(q):
            return pltpu.make_async_copy(tb.at[q % 2], terms.at[:, col(q)], wsem.at[1 + q % 2])

        def own_terms(r, q):
            k = G - 1 - r
            part = dot(dpre[0, pl.ds(2 * k, 2)].reshape(2 * R, F), w2[:, col(q)], 1, 0)
            own[...] = part.reshape(2, R, DC)

        sib_arrive(0, 0)
        sib_load(0, 0).start()
        own_terms(0, 0)

        @pl.loop(0, G)
        def _(r):
            @pl.loop(0, SUB)
            def _(q):
                @pl.when((r == 0) & (q == 0))
                def _():
                    got[...] = jnp.zeros_like(got)

                sib_load(r, q).wait()

                @pl.when(r == 0)
                def _():
                    out[0, q, 0] = (own[0] + gsib[q % 2, 0].astype(F32)).astype(BF16)
                    for i in range(2):
                        rs_half(i, q).start()

                    @pl.when(q >= 2)
                    def _():
                        term_out(q - 2).wait()

                    tb[q % 2] = own[1] + gsib[q % 2, 1].astype(F32)
                    term_out(q).start()

                    @pl.when(q == SUB - 1)
                    def _():
                        pump(2 * G - 1, 0)

                @pl.when(r == 2)
                def _():
                    left(out.at[0, q, 0], rss.at[0, q])

                @pl.when(r > 2)
                def _():
                    left(out.at[r % 2, q], rss.at[r % 2, q])

                @pl.when((r == G - 1) & (q == SUB - 1))
                def _():
                    arrived(late, rsr.at[G - 2, SUB - 1])

                for i in range(2):
                    @pl.when(r == 1)
                    def _():
                        got_half(i, q).wait()

                    end = (r == G - 1) & (q == SUB - 1)

                    @pl.when((r > 1) & jnp.logical_not(end))
                    def _():
                        got_load(r, i, q).wait()

                    @pl.when((r > 0) & jnp.logical_not(end))
                    def _():
                        out[r % 2, q, i] = (own[i] + gsib[q % 2, i].astype(F32) + got[q % 2, i].astype(F32)).astype(BF16)

                    @pl.when(end)
                    def _():
                        out[r % 2, q, i] = (own[i] + gsib[q % 2, i].astype(F32) + late[i].astype(F32)).astype(BF16)

                    to_late = (r == G - 2) & (q == SUB - 1)

                    @pl.when((r > 0) & (r < G - 1) & jnp.logical_not(to_late))
                    def _():
                        rs_copy(r, i, q).start()

                    @pl.when(to_late)
                    def _():
                        rs_late(i).start()

                    @pl.when((r == G - 1) & (q == 0))
                    def _():
                        rs_fill(i).start()
                        snd_out(i, 0).start()

                    @pl.when((r == G - 1) & (q > 0))
                    def _():
                        snd_out(i, q).start()

                @pl.when((r < G - 1) | (q < SUB - 1))
                def _():
                    q1 = (q + 1) % SUB
                    r1 = r + (q + 1) // SUB
                    sib_arrive(r1, q1)
                    sib_load(r1, q1).start()
                    own_terms(r1, q1)

                    @pl.when(r1 == 1)
                    def _():
                        arrived(rsb.at[0, 0, 0], rsr.at[0, q1])
                        for i in range(2):
                            got_half(i, q1).start()

                    @pl.when((r1 > 1) & ((r1 < G - 1) | (q1 < SUB - 1)))
                    def _():
                        arrived(rsb.at[0, 0], rsr.at[r1 - 1, q1])
                        for i in range(2):
                            got_load(r1, i, q1).start()

                extra = jnp.where(r < G - 1, 1, 0)
                base = (SUB + 1) * (r - 1) + q + jnp.where(q > 0, extra, 0)
                count = jnp.where(q == 0, 1 + extra, 1)

                @pl.loop(0, jnp.where(r == 0, 0, jnp.minimum(count, NT - base)))
                def _(jj):
                    i = base + jj

                    @pl.when(i == 0)
                    def _():
                        for lot in range(2):
                            arrived(gb.at[1, pl.ds(0, S // 2)], d2r.at[S // 2 + 1 + lot])

                        x_load(0).start()

                    x_load(i).wait()

                    @pl.when(i == NT // 2)
                    def _():
                        sent()

                    @pl.when(i + 1 < NT)
                    def _():
                        x_load(i + 1).start()

                    @pl.when(i >= 2)
                    def _():
                        e_out(i - 2).wait()

                    eo[i % 2] = dot(xt[i % 2].reshape(2 * S * R, TILE), dpre[...].reshape(2 * S * R, F), 0, 0).astype(BF16)
                    e_out(i).start()

        for i in range(NT - 2, NT):
            e_out(i).wait()
        for q in range(SUB):
            left(out.at[0, q], rss.at[(G - 2) % 2, q])
        for q in range(SUB - 2, SUB):
            term_out(q).wait()
        for i, snd in enumerate((snd1, snd0)):
            pltpu.make_async_copy(snd, snd, fsem.at[i]).wait()
        left(filled, xsem.at[0])
        arrived(filled, xsem.at[1])

    pl.run_scoped(p3, pltpu.VMEM((2, R, DC), F32), pltpu.VMEM((2, 2, S, R, TILE), BF16), pltpu.VMEM((2, TILE, F), BF16),
                  pltpu.VMEM((2, 2, R, DC), BF16), pltpu.VMEM((2, 2, R, DC), BF16), pltpu.VMEM((2, SUB, 2, R, DC), BF16),
                  pltpu.VMEM((2, R, DC), F32))


def copy_kernel(a, b, a2, b2, abuf, bbuf, isem, osem):
    get, put = [], []
    for src, dst, buf, sizes in ((a, a2, abuf, (4, 12, 16)), (b, b2, bbuf, (16, 12, 4))):
        unit, row = src.shape[0] // sum(sizes), 0
        for size in sizes:
            at = pl.ds(row, size * unit)
            row += size * unit
            get.append(pltpu.make_async_copy(src.at[at], buf.at[at], isem.at[len(get)]))
            put.append(pltpu.make_async_copy(buf.at[at], dst.at[at], osem.at[len(put)]))
    for c in get:
        c.start()
    for g, p in zip(get, put):
        g.wait()
        p.start()
    for c in put:
        c.wait()


def copied(a, b):
    dma = pltpu.SemaphoreType.DMA
    return pl.pallas_call(
        copy_kernel,
        out_shape=[jax.ShapeDtypeStruct(t.shape, t.dtype) for t in (a, b)],
        in_specs=[pl.BlockSpec(memory_space=pl.ANY)] * 2,
        out_specs=[pl.BlockSpec(memory_space=pl.ANY)] * 2,
        scratch_shapes=[pltpu.VMEM(t.shape, t.dtype) for t in (a, b)] + [dma((6,))] * 2,
        compiler_params=pltpu.CompilerParams(vmem_limit_bytes=48 * 2**20),
        cost_estimate=pl.CostEstimate(flops=8 * 10**9, bytes_accessed=8 * a.size, transcendentals=0),
        name="copy_out",
    )(a, b)


def add_kernel(a, b, c, f, o, v, sem):
    n, parts = f.shape[2], sem.shape[0]
    wide = a.shape[1] // parts
    out = []
    for i in range(parts):
        at = i * wide
        if i == 0:
            v[:, :n] = (a[:, :n] + f[1].astype(F32) + f[0].astype(F32)).astype(BF16)
            at = n
        cols, part = slice(at, (i + 1) * wide), slice(at - n, (i + 1) * wide - n)
        v[:, cols] = (a[:, cols] + b[:, part].astype(F32) + c[:, part].astype(F32)).astype(BF16)
        done = pl.ds(i * wide, wide)
        out.append(pltpu.make_async_copy(v.at[:, done], o.at[:, done], sem.at[i]))
        out[-1].start()
    for copy in out:
        copy.wait()


def added(term, ahead, back, filled):
    whole = pl.BlockSpec(memory_space=pltpu.VMEM)
    return pl.pallas_call(
        add_kernel, in_specs=[whole] * 4, out_specs=pl.BlockSpec(memory_space=pl.ANY), out_shape=jax.ShapeDtypeStruct(term.shape, BF16),
        scratch_shapes=[pltpu.VMEM(term.shape, BF16), pltpu.SemaphoreType.DMA((4,))], name="last_add",
        compiler_params=pltpu.CompilerParams(vmem_limit_bytes=16 * 2**20),
    )(term, ahead, back, filled)


def solution(mesh):
    n = mesh.shape["tp"]
    S = n // 2
    G = S // 2
    perms = ring_perms(n)

    def step(x, dy, pre, w_in, w_down):
        R, D = x.shape
        F = pre.shape[1]
        sds = jax.ShapeDtypeStruct
        dma = pltpu.SemaphoreType.DMA
        *sums, term, filled, dw_in, dw_down, _, _, _ = pl.pallas_call(
            functools.partial(kernel, n),
            out_shape=(
                sds((R, D - FILL), BF16), sds((R, D - FILL), BF16), sds((R, D), F32), sds((2, R, FILL), BF16), sds((D, F), BF16), sds((F, D), BF16),
                sds((2, 2 * S, R, D), BF16), sds((G - 1, SUB, 2, R, D // SUB), BF16), sds((G, SUB, 2, R, D // SUB), BF16),
            ),
            in_specs=[pl.BlockSpec(memory_space=pl.ANY)] * 5,
            out_specs=[pl.BlockSpec(memory_space=pl.ANY)] * 9,
            scratch_shapes=[
                pltpu.VMEM((2, S, R, F), BF16), pltpu.VMEM((F, D), BF16), pltpu.VMEM((2, R, D // SUB), BF16),
                dma((2 * G, 2)), dma((4,)), dma((G + 3,)), dma((4,)), dma((G - 1, SUB)), dma((2, SUB)), dma((G,)), dma((2,)),
                dma((3,)), dma((2,)), dma((2,)), dma((2,)), dma((2,)), dma((2,)), dma((2, 2)), dma((2,)),
            ],
            compiler_params=pltpu.CompilerParams(collective_id=0, has_side_effects=True, vmem_limit_bytes=VMEM_LIMIT),
            name="mlp_backward",
        )(x, dy, pre, w_in, w_down)
        dw_in, dw_down = copied(dw_in, dw_down)
        ahead, back = (lax.ppermute(a, "tp", perm) for a, perm in zip(sums, perms))
        return added(term, ahead, back, filled), dw_in, dw_down

    rows, cols = P(("dp", "tp"), None), P("dp", "tp")
    return jax.shard_map(
        step, mesh=mesh, in_specs=(rows, rows, cols, P(None, "tp"), P("tp", None)),
        out_specs=(rows, cols, rows), check_vma=False,
    )
```

```python
import functools
import math

import jax
import jax.numpy as jnp
from jax import lax
from jax.experimental import pallas as pl
from jax.experimental.pallas import tpu as pltpu
from jax.sharding import PartitionSpec as P

MESH = pl.DeviceIdType.MESH
F32, BF16 = jnp.float32, jnp.bfloat16
SUB = 4
TILE = 256
FILL = 512
VMEM_LIMIT = 67043328


def ring_pos(side, chip, ring):
    a, b = chip // side, chip % side
    return jnp.where(ring == 0, a, b) * side + (a + b) % side


def ring_chip(side, pos, ring):
    pos = (pos + side * side) % (side * side)
    major = pos // side
    minor = (pos % side - major + side) % side
    return jnp.where(ring == 0, major * side + minor, minor * side + major)


def ring_perms(n):
    S = n // 2
    side = math.isqrt(S)
    with jax.ensure_compile_time_eval():
        ring = [[int(ring_chip(side, p, c)) * 2 + c for p in range(S)] for c in range(2)]
    return [[(r[p], r[(p + d) % S]) for r in ring for p in range(S)] for d in (1, -1)]


def dot(a, b, ca, cb):
    return lax.dot_general(a, b, (((ca,), (cb,)), ((), ())), preferred_element_type=F32)


def gelu_and_slope(p):
    c = math.sqrt(2.0 / math.pi)
    sq = p * p
    t = jnp.tanh(c * (p + 0.044715 * (sq * p)))
    cdf = 0.5 * (1.0 + t)
    slope = cdf + p * (cdf * (1.0 - t)) * (c * (1.0 + 3 * 0.044715 * sq))
    return p * cdf, slope


def kernel(n, x, dy, pre, w_in, w_down, snd0, snd1, terms, filled, dw_in, dw_down, gb, rsb, sbb, dpre, w2, late,
           agr, ags, d2r, d2s, rsr, rss, sbr, sbs, wsem, psem, osem, lsem, tsem, fsem, gsem, xsem):
    S = n // 2
    G = S // 2
    side = math.isqrt(S)
    R, D = x.shape
    H, F = R // 2, pre.shape[1]
    DC, FC = D // SUB, F // SUB
    NT = D // TILE
    me = lax.axis_index("tp")
    chip, core = me // 2, me % 2
    pos, pos2 = ring_pos(side, chip, core), ring_pos(side, chip, 1 - core)
    nxt = [ring_chip(side, pos + 1, core) * 2 + core, ring_chip(side, pos - 1, core) * 2 + core]
    sib = chip * 2 + 1 - core

    def remote(src, dst, ssem, rsem, dev):
        return pltpu.make_async_remote_copy(src, dst, ssem, rsem, device_id={"tp": dev}, device_id_type=MESH)

    def arrived(ref, sem):
        remote(ref, ref, rss.at[0, 0], sem, sib).wait_recv()

    def left(ref, sem):
        remote(ref, ref, sem, rsr.at[0, 0], sib).wait_send()

    def land(v, d):
        return S * (v // G) + jnp.where(v % G == G - 1, S - 2, 2 * (v % G) + d)

    def half_of(e, d):
        q = (e + d) % 2
        return pl.ds(q * H if isinstance(q, int) else pl.multiple_of(q * H, H), H)

    def ag_copy(v, d, e, src=None):
        rows = half_of(e, d)
        slot = S * (v // G) + jnp.where(v % G == 0, S - 1, 2 * (v % G - 1) + d)
        src = gb.at[0, slot, rows] if src is None else src.at[rows]
        return remote(src, gb.at[0, land(v, d), rows], ags.at[v // (G // 2)], agr.at[v, e], nxt[d])

    def handed(w):
        return jnp.where(w < S - 2, w // 2, jnp.where(w < S, w - S // 2 + 1, S // 2 + 1 + (w - S) // (S // 2)))

    def hand(w, rows=None, src=None):
        ref = gb.at[0, w] if src is None else src
        dst = gb.at[1, w]
        if rows is not None:
            ref, dst = ref.at[rows], dst.at[rows]
        return remote(ref, dst, d2s.at[w // (S // 2)], d2r.at[handed(w)], sib)

    def pump(v, e):
        @pl.when((v % G < G - 1) | (e == 0))
        def _():
            arrived(gb.at[0, 0], agr.at[v, e])

            @pl.when((v % G < G - 2) | ((v % G == G - 2) & (e == 0)))
            def _():
                for d in range(2):
                    ag_copy(v + 1, d, e).start()

            @pl.when((v == G - 2) & (e == 1))
            def _():
                for p in range(2):
                    for d in range(2):
                        ag_copy(G, d, p).start()

            for d in range(2):
                hand(land(v, d), half_of(e, d)).start()

    bar = pltpu.get_barrier_semaphore()
    for dev in (*nxt, sib):
        pl.semaphore_signal(bar, inc=1, device_id={"tp": dev}, device_id_type=MESH)
    pl.semaphore_wait(bar, 3)
    for e in range(2):
        for d in range(2):
            ag_copy(0, d, e, dy).start()
    hand(S - 1, src=dy).start()
    hand(2 * S - 1, src=x).start()

    def first(hT):
        def p1(w1, a, prb, wst):
            load_w1 = pltpu.make_async_copy(w_down, w1, wsem.at[0])
            own = [pltpu.make_async_copy(src, a.at[0, i], lsem.at[i]) for i, src in enumerate((dy, x))]
            put = [pltpu.make_async_copy(a.at[0, i], gb.at[0, (i + 1) * S - 1], lsem.at[i]) for i in range(2)]
            for c in own:
                c.start()
            load_w1.start()
            for o, c in zip(own, put):
                o.wait()
                c.start()
            for c in put:
                c.wait()

            def slot_of(u):
                return (u + S - 1) % S

            def loads(u):
                e, b = slot_of(u), u % 2
                out = [pltpu.make_async_copy(gb.at[:, e], a.at[b], lsem.at[b])]
                away = jnp.where(e == S - 1, 0, jnp.where(e == S - 2, S // 2, jnp.where(e % 2 == 0, S - 1 - e // 2, e // 2 + 1)))
                for h, (ps, cr) in enumerate(((pos, core), (pos2, 1 - core))):
                    row = pl.multiple_of((ring_chip(side, ps + away - S, cr) * 2 + cr) * R, R)
                    out.append(pltpu.make_async_copy(pre.at[pl.ds(row, R)], prb.at[b, h], psem.at[b]))
                rows = pl.ds(pl.multiple_of(u * (D // S), D // S), D // S)
                out.append(pltpu.make_async_copy(w_in.at[rows], wst, wsem.at[1]))
                return out

            def fetch(u):
                @pl.when((u % 2 == 1) & (u < S - 1))
                def _():
                    arrived(gb.at[1, pl.ds(0, 2)], d2r.at[handed(slot_of(u))])

                @pl.when((u == 0) | (u == S - 1))
                def _():
                    arrived(gb.at[1, 0], d2r.at[handed(slot_of(u))])

                for c in loads(u):
                    c.start()

            def fetched(u):
                b = u % 2
                for ref, sem in ((a.at[b], lsem.at[b]), (prb.at[b], psem.at[b]), (wst, wsem.at[1])):
                    pltpu.make_async_copy(ref, ref, sem).wait()

            fetch(0)
            load_w1.wait()

            @pl.loop(0, G + 1)
            def _(v):
                @pl.loop(0, 2)
                def _(half):
                    u = 2 * v - 1 + half
                    busy = (u >= 0) & (u < S) & ((v > 0) | (half == 1))

                    @pl.loop(0, SUB)
                    def _(j):
                        @pl.when(j == 0)
                        def _():
                            pump(v, half)

                        @pl.when(busy)
                        def _():
                            b = u % 2

                            @pl.when(j == 0)
                            def _():
                                fetched(u)
                                w2[:, pl.ds(pl.multiple_of(u * (D // S), D // S), D // S)] = wst[...].T

                                @pl.when((half == 0) & (u + 1 < S))
                                def _():
                                    fetch(u + 1)

                            cols = pl.ds(pl.multiple_of(j * FC, FC), FC)
                            dh = dot(a[b].reshape(2 * R, D), w1[cols, :], 1, 1)
                            for h in range(2):
                                hid, slope = gelu_and_slope(prb[b, h, :, cols].astype(F32))
                                dpre[h, slot_of(u), :, cols] = (dh[h * R : (h + 1) * R] * slope).astype(BF16)
                                tok = pl.ds(pl.multiple_of((h * S + slot_of(u)) * R, R), R)
                                hT[cols, tok] = hid.T.astype(BF16)

                            @pl.when((j == SUB - 1) & (half == 1) & (u + 1 < S))
                            def _():
                                fetch(u + 1)

        pl.run_scoped(p1, pltpu.VMEM((F, D), BF16), pltpu.VMEM((2, 2, R, D), BF16), pltpu.VMEM((2, 2, R, F), BF16),
                      pltpu.VMEM((D // S, F), BF16))

        def p2(tile, dout, sst):
            def tile_load(i):
                cols = pl.ds(pl.multiple_of(i * TILE, TILE), TILE)
                return pltpu.make_async_copy(gb.at[:, pl.ds(0, S), :, cols], tile.at[i % 2], tsem.at[i % 2])

            def tile_out(i):
                cols = pl.ds(pl.multiple_of(i * TILE, TILE), TILE)
                return pltpu.make_async_copy(dout.at[i % 2], dw_down.at[:, cols], osem.at[i % 2])

            def sib_copy(k, c):
                return remote(sst.at[k % 2, c], sbb.at[k, c], sbs.at[k % 2], sbr.at[k], sib)

            tile_load(0).start()

            @pl.loop(0, S)
            def _(g):
                def step(w):
                    @pl.when(w % 4 == 3)
                    def _():
                        pump(G + 1 + w // 8, (w // 4) % 2)

                step(3 * g)

                @pl.loop(0, 2)
                def _(j):
                    k, c = G - 1 - g // 2, (g % 2) * 2 + j

                    @pl.when((g >= 4) & (c == 0))
                    def _():
                        left(sst.at[k % 2], sbs.at[k % 2])

                    part = dot(dpre[1, pl.ds(2 * k, 2)].reshape(2 * R, F), w2[:, pl.ds(pl.multiple_of(c * DC, DC), DC)], 1, 0)
                    sst[k % 2, c] = part.astype(BF16).reshape(2, R, DC)
                    sib_copy(k, c).start()

                @pl.loop(0, 2)
                def _(j):
                    step(3 * g + 1 + j)
                    i = 2 * g + j
                    tile_load(i).wait()

                    @pl.when(i + 1 < NT)
                    def _():
                        tile_load(i + 1).start()

                    @pl.when(i >= 2)
                    def _():
                        tile_out(i - 2).wait()

                    dout[i % 2] = dot(hT[...], tile[i % 2].reshape(2 * S * R, TILE), 1, 0).astype(BF16)
                    tile_out(i).start()

            for i in range(NT - 2, NT):
                tile_out(i).wait()

            for k in range(2):
                left(sst.at[k], sbs.at[k])

        pl.run_scoped(p2, pltpu.VMEM((2, 2, S, R, TILE), BF16), pltpu.VMEM((2, F, TILE), BF16), pltpu.VMEM((2, SUB, 2, R, DC), BF16))

    pl.run_scoped(first, pltpu.VMEM((F, 2 * S * R), BF16))

    def sent():
        for v in range(4):
            left(gb.at[0, pl.ds(0, S // 2 - v % 2)], ags.at[v])
            left(gb.at[0, pl.ds(0, S // 2)], d2s.at[v])

    def p3(own, xt, eo, got, gsib, out, tb):
        def x_load(i):
            cols = pl.ds(pl.multiple_of(i * TILE, TILE), TILE)
            return pltpu.make_async_copy(gb.at[:, pl.ds(S, S), :, cols], xt.at[i % 2], tsem.at[i % 2])

        def e_out(i):
            return pltpu.make_async_copy(eo.at[i % 2], dw_in.at[pl.ds(pl.multiple_of(i * TILE, TILE), TILE)], osem.at[i % 2])

        def rs_copy(r, i, q):
            return remote(out.at[r % 2, q, i], rsb.at[r, q, i], rss.at[r % 2, q], rsr.at[r, q], nxt[1 - i])

        def rs_late(i):
            r, q = G - 2, SUB - 1
            return remote(out.at[r % 2, q, i], late.at[i], rss.at[r % 2, q], rsr.at[r, q], nxt[1 - i])

        def rs_fill(i):
            return remote(out.at[(G - 1) % 2, 0, i, :, pl.ds(0, FILL)], filled.at[i], xsem.at[0], xsem.at[1], nxt[1 - i])

        def rs_half(i, q):
            rows = pl.ds(H * (1 - i), H)
            return remote(out.at[0, q, 0, rows], rsb.at[0, q, i, rows], rss.at[0, q], rsr.at[0, q], nxt[1 - i])

        def got_load(r, i, q):
            return pltpu.make_async_copy(rsb.at[r - 1, q, i], got.at[q % 2, i], gsem.at[q % 2, i])

        def got_half(i, q):
            rows = pl.ds(H * (1 - i), H)
            return pltpu.make_async_copy(rsb.at[0, q, i, rows], got.at[q % 2, i, rows], gsem.at[q % 2, i])

        def sib_load(r, q):
            return pltpu.make_async_copy(sbb.at[G - 1 - r, q], gsib.at[q % 2], psem.at[q % 2])

        def sib_arrive(r, q):
            @pl.when(q == 0)
            def _():
                arrived(sbb.at[G - 1 - r], sbr.at[G - 1 - r])

        def col(q):
            return pl.ds(pl.multiple_of(q * DC, DC), DC)

        def snd_out(i, q):
            if isinstance(q, int) and q == 0:
                cols, to = pl.ds(FILL, DC - FILL), pl.ds(0, DC - FILL)
            else:
                cols, to = pl.ds(0, DC), pl.ds(pl.multiple_of(q * DC - FILL, FILL), DC)
            return pltpu.make_async_copy(out.at[(G - 1) % 2, q, i, :, cols], (snd1, snd0)[i].at[:, to], fsem.at[i])

        def term_out(q):
            return pltpu.make_async_copy(tb.at[q % 2], terms.at[:, col(q)], wsem.at[1 + q % 2])

        def own_terms(r, q):
            k = G - 1 - r
            part = dot(dpre[0, pl.ds(2 * k, 2)].reshape(2 * R, F), w2[:, col(q)], 1, 0)
            own[...] = part.reshape(2, R, DC)

        sib_arrive(0, 0)
        sib_load(0, 0).start()
        own_terms(0, 0)

        @pl.loop(0, G)
        def _(r):
            @pl.loop(0, SUB)
            def _(q):
                @pl.when((r == 0) & (q == 0))
                def _():
                    got[...] = jnp.zeros_like(got)

                sib_load(r, q).wait()

                @pl.when(r == 0)
                def _():
                    out[0, q, 0] = (own[0] + gsib[q % 2, 0].astype(F32)).astype(BF16)
                    for i in range(2):
                        rs_half(i, q).start()

                    @pl.when(q >= 2)
                    def _():
                        term_out(q - 2).wait()

                    tb[q % 2] = own[1] + gsib[q % 2, 1].astype(F32)
                    term_out(q).start()

                    @pl.when(q == SUB - 1)
                    def _():
                        pump(2 * G - 1, 0)

                @pl.when(r == 2)
                def _():
                    left(out.at[0, q, 0], rss.at[0, q])

                @pl.when(r > 2)
                def _():
                    left(out.at[r % 2, q], rss.at[r % 2, q])

                @pl.when((r == G - 1) & (q == SUB - 1))
                def _():
                    arrived(late, rsr.at[G - 2, SUB - 1])

                for i in range(2):
                    @pl.when(r == 1)
                    def _():
                        got_half(i, q).wait()

                    end = (r == G - 1) & (q == SUB - 1)

                    @pl.when((r > 1) & jnp.logical_not(end))
                    def _():
                        got_load(r, i, q).wait()

                    @pl.when((r > 0) & jnp.logical_not(end))
                    def _():
                        out[r % 2, q, i] = (own[i] + gsib[q % 2, i].astype(F32) + got[q % 2, i].astype(F32)).astype(BF16)

                    @pl.when(end)
                    def _():
                        out[r % 2, q, i] = (own[i] + gsib[q % 2, i].astype(F32) + late[i].astype(F32)).astype(BF16)

                    to_late = (r == G - 2) & (q == SUB - 1)

                    @pl.when((r > 0) & (r < G - 1) & jnp.logical_not(to_late))
                    def _():
                        rs_copy(r, i, q).start()

                    @pl.when(to_late)
                    def _():
                        rs_late(i).start()

                    @pl.when((r == G - 1) & (q == 0))
                    def _():
                        rs_fill(i).start()
                        snd_out(i, 0).start()

                    @pl.when((r == G - 1) & (q > 0))
                    def _():
                        snd_out(i, q).start()

                @pl.when((r < G - 1) | (q < SUB - 1))
                def _():
                    q1 = (q + 1) % SUB
                    r1 = r + (q + 1) // SUB
                    sib_arrive(r1, q1)
                    sib_load(r1, q1).start()
                    own_terms(r1, q1)

                    @pl.when(r1 == 1)
                    def _():
                        arrived(rsb.at[0, 0, 0], rsr.at[0, q1])
                        for i in range(2):
                            got_half(i, q1).start()

                    @pl.when((r1 > 1) & ((r1 < G - 1) | (q1 < SUB - 1)))
                    def _():
                        arrived(rsb.at[0, 0], rsr.at[r1 - 1, q1])
                        for i in range(2):
                            got_load(r1, i, q1).start()

                extra = jnp.where(r < G - 1, 1, 0)
                base = (SUB + 1) * (r - 1) + q + jnp.where(q > 0, extra, 0)
                count = jnp.where(q == 0, 1 + extra, 1)

                @pl.loop(0, jnp.where(r == 0, 0, jnp.minimum(count, NT - base)))
                def _(jj):
                    i = base + jj

                    @pl.when(i == 0)
                    def _():
                        for lot in range(2):
                            arrived(gb.at[1, pl.ds(0, S // 2)], d2r.at[S // 2 + 1 + lot])

                        x_load(0).start()

                    x_load(i).wait()

                    @pl.when(i == NT // 2)
                    def _():
                        sent()

                    @pl.when(i + 1 < NT)
                    def _():
                        x_load(i + 1).start()

                    @pl.when(i >= 2)
                    def _():
                        e_out(i - 2).wait()

                    eo[i % 2] = dot(xt[i % 2].reshape(2 * S * R, TILE), dpre[...].reshape(2 * S * R, F), 0, 0).astype(BF16)
                    e_out(i).start()

        for i in range(NT - 2, NT):
            e_out(i).wait()
        for q in range(SUB):
            left(out.at[0, q], rss.at[(G - 2) % 2, q])
        for q in range(SUB - 2, SUB):
            term_out(q).wait()
        for i, snd in enumerate((snd1, snd0)):
            pltpu.make_async_copy(snd, snd, fsem.at[i]).wait()
        left(filled, xsem.at[0])
        arrived(filled, xsem.at[1])

    pl.run_scoped(p3, pltpu.VMEM((2, R, DC), F32), pltpu.VMEM((2, 2, S, R, TILE), BF16), pltpu.VMEM((2, TILE, F), BF16),
                  pltpu.VMEM((2, 2, R, DC), BF16), pltpu.VMEM((2, 2, R, DC), BF16), pltpu.VMEM((2, SUB, 2, R, DC), BF16),
                  pltpu.VMEM((2, R, DC), F32))


def copy_kernel(a, b, a2, b2, abuf, bbuf, isem, osem):
    get, put = [], []
    for src, dst, buf, sizes in ((a, a2, abuf, (4, 12, 16)), (b, b2, bbuf, (12, 12, 8))):
        unit, row = src.shape[0] // sum(sizes), 0
        for size in sizes:
            at = pl.ds(row, size * unit)
            row += size * unit
            get.append(pltpu.make_async_copy(src.at[at], buf.at[at], isem.at[len(get)]))
            put.append(pltpu.make_async_copy(buf.at[at], dst.at[at], osem.at[len(put)]))
    for c in get:
        c.start()
    for g, p in zip(get, put):
        g.wait()
        p.start()
    for c in put:
        c.wait()


def copied(a, b):
    dma = pltpu.SemaphoreType.DMA
    return pl.pallas_call(
        copy_kernel,
        out_shape=[jax.ShapeDtypeStruct(t.shape, t.dtype) for t in (a, b)],
        in_specs=[pl.BlockSpec(memory_space=pl.ANY)] * 2,
        out_specs=[pl.BlockSpec(memory_space=pl.ANY)] * 2,
        scratch_shapes=[pltpu.VMEM(t.shape, t.dtype) for t in (a, b)] + [dma((6,))] * 2,
        compiler_params=pltpu.CompilerParams(vmem_limit_bytes=48 * 2**20),
        cost_estimate=pl.CostEstimate(flops=8 * 10**9, bytes_accessed=8 * a.size, transcendentals=0),
        name="copy_out",
    )(a, b)


def add_kernel(a, b, c, f, o, v, sem):
    n, parts = f.shape[2], sem.shape[0]
    wide = a.shape[1] // parts
    out = []
    for i in range(parts):
        at = i * wide
        if i == 0:
            v[:, :n] = (a[:, :n] + f[1].astype(F32) + f[0].astype(F32)).astype(BF16)
            at = n
        cols, part = slice(at, (i + 1) * wide), slice(at - n, (i + 1) * wide - n)
        v[:, cols] = (a[:, cols] + b[:, part].astype(F32) + c[:, part].astype(F32)).astype(BF16)
        done = pl.ds(i * wide, wide)
        out.append(pltpu.make_async_copy(v.at[:, done], o.at[:, done], sem.at[i]))
        out[-1].start()
    for copy in out:
        copy.wait()


def added(term, ahead, back, filled):
    whole = pl.BlockSpec(memory_space=pltpu.VMEM)
    return pl.pallas_call(
        add_kernel, in_specs=[whole] * 4, out_specs=pl.BlockSpec(memory_space=pl.ANY), out_shape=jax.ShapeDtypeStruct(term.shape, BF16),
        scratch_shapes=[pltpu.VMEM(term.shape, BF16), pltpu.SemaphoreType.DMA((4,))], name="last_add",
        compiler_params=pltpu.CompilerParams(vmem_limit_bytes=16 * 2**20),
    )(term, ahead, back, filled)


def solution(mesh):
    n = mesh.shape["tp"]
    S = n // 2
    G = S // 2
    perms = ring_perms(n)

    def step(x, dy, pre, w_in, w_down):
        R, D = x.shape
        F = pre.shape[1]
        sds = jax.ShapeDtypeStruct
        dma = pltpu.SemaphoreType.DMA
        *sums, term, filled, dw_in, dw_down, _, _, _ = pl.pallas_call(
            functools.partial(kernel, n),
            out_shape=(
                sds((R, D - FILL), BF16), sds((R, D - FILL), BF16), sds((R, D), F32), sds((2, R, FILL), BF16), sds((D, F), BF16), sds((F, D), BF16),
                sds((2, 2 * S, R, D), BF16), sds((G - 1, SUB, 2, R, D // SUB), BF16), sds((G, SUB, 2, R, D // SUB), BF16),
            ),
            in_specs=[pl.BlockSpec(memory_space=pl.ANY)] * 5,
            out_specs=[pl.BlockSpec(memory_space=pl.ANY)] * 9,
            scratch_shapes=[
                pltpu.VMEM((2, S, R, F), BF16), pltpu.VMEM((F, D), BF16), pltpu.VMEM((2, R, D // SUB), BF16),
                dma((2 * G, 2)), dma((4,)), dma((G + 3,)), dma((4,)), dma((G - 1, SUB)), dma((2, SUB)), dma((G,)), dma((2,)),
                dma((3,)), dma((2,)), dma((2,)), dma((2,)), dma((2,)), dma((2,)), dma((2, 2)), dma((2,)),
            ],
            compiler_params=pltpu.CompilerParams(collective_id=0, has_side_effects=True, vmem_limit_bytes=VMEM_LIMIT),
            name="mlp_backward",
        )(x, dy, pre, w_in, w_down)
        dw_in, dw_down = copied(dw_in, dw_down)
        ahead, back = (lax.ppermute(a, "tp", perm) for a, perm in zip(sums, perms))
        return added(term, ahead, back, filled), dw_in, dw_down

    rows, cols = P(("dp", "tp"), None), P("dp", "tp")
    return jax.shard_map(
        step, mesh=mesh, in_specs=(rows, rows, cols, P(None, "tp"), P("tp", None)),
        out_specs=(rows, cols, rows), check_vma=False,
    )
```
